256 devices in a mesh: kx: 16 (over z, x_lo), cz: 16 (over y, x_hi, core).
Axes of the slice: x: 4 (x_hi: 2, x_lo: 2; x = x_hi * 2 + x_lo), y: 4, z: 8, core: 2. Of those that a mesh axis runs over, the one named last changes fastest.
Arguments:
- field_modes: bfloat16 [512, 4, 12288], P('cz', None, 'kx'), may hold values from -6 to 6
- cotangent: bfloat16 [512, 4, 12288], P('cz', None, 'kx'), may hold values from -6 to 6
Outputs:
- mode_gradient: bfloat16 [512, 4, 12288], P('cz', None, 'kx')
The draws below stay inside these ranges and needn't reach their ends.
All inputs are finite; a program needn't handle non-finite values.
Results may differ from the reference program's by a relative error of at most 0.009.
Values may be sent and summed in bfloat16 or wider, within the bound.
A program may use at most 128 MiB of HBM per device.

```python
import math
import jax
import jax.numpy as jnp
from jax import lax

FIELDS = 4
NZ = 512
MZ = 768
NX = 768
Y = 16


def steps_of(key, dims, pieces, smallest, largest):
    gain, own = 1.0, jax.random.fold_in(key, 6)
    for axis_at, shards_of in pieces:
        heights = jnp.exp(jax.random.uniform(jax.random.fold_in(own, axis_at), (shards_of,), jnp.float32, smallest / len(pieces), largest / len(pieces)))
        gain = gain * jnp.repeat(heights, dims[axis_at] // shards_of).reshape([-1 if axis == axis_at else 1 for axis in range(len(dims))])
    return gain


def normal_values(rng, shape, spread, bound, cuts=(), kind=jnp.bfloat16):
    factor_of = steps_of(rng, shape, cuts, -0.22, 0.18) if cuts else 1.0
    drawn = jax.random.normal(rng, shape, jnp.float32) * spread * factor_of
    return jnp.minimum(jnp.maximum(drawn, -bound), bound).astype(kind)


def setup_inputs(seed: int = 0) -> dict:
    key_of = jax.random.split(jax.random.key(seed), 3)
    return {
        "field_modes": normal_values(key_of[0], (NZ, FIELDS, NX * Y), 1.0, 6.0, ((0, 16), (2, 16))),
        "cotangent": normal_values(key_of[1], (NZ, FIELDS, NX * Y), 1.0, 6.0, ((0, 16), (2, 16))),
    }


def cosine_table():
    row_index = jnp.arange(MZ, dtype=jnp.int32)
    col_index = jnp.arange(NZ, dtype=jnp.int32)
    position = col_index[None, :] * (2 * row_index[:, None] + 1) % (4 * MZ)
    return jnp.cos(jnp.pi * position.astype(jnp.float32) / (2 * MZ))

def hartley_table():
    points = jnp.arange(NX, dtype=jnp.int32)
    position = points[:, None] * points[None, :] % NX
    phases = 2.0 * jnp.pi * position.astype(jnp.float32) / NX
    return ((jnp.cos(phases) + jnp.sin(phases)) / math.sqrt(NX)).astype(jnp.bfloat16)

def product_gradient(fields, adjoint):
    vertical = fields[2]
    return jnp.stack([adjoint[0] * vertical, adjoint[1] * vertical, adjoint[0] * fields[0] + adjoint[1] * fields[1] + 2.0 * adjoint[2] * vertical + adjoint[3] * fields[3], adjoint[3] * vertical]).astype(jnp.bfloat16)

def reference(field_modes, cotangent):
    highest = lax.Precision.HIGHEST
    field_grid = field_modes.reshape(NZ, FIELDS, NX, Y)
    cotangent_grid = cotangent.reshape(NZ, FIELDS, NX, Y)
    cosines = cosine_table()
    synthesis_full = (cosines * math.sqrt(2.0 / NZ)).astype(jnp.bfloat16).astype(jnp.float32)
    projection_full = (cosines * math.sqrt(2.0 / MZ)).astype(jnp.bfloat16).astype(jnp.float32)
    hartley_full = hartley_table().astype(jnp.float32)
    block_rows = 8
    block_count = Y // block_rows

    def one_block(position):
        first_row = position * block_rows
        mode_block = lax.dynamic_slice_in_dim(field_grid, first_row, block_rows, 3).astype(jnp.float32)
        adjoint_block = lax.dynamic_slice_in_dim(cotangent_grid, first_row, block_rows, 3).astype(jnp.float32)
        lifted_fields = jnp.einsum('zk,kfmy->fzmy', synthesis_full, mode_block, precision=highest).astype(jnp.bfloat16).astype(jnp.float32)
        lifted_adjoint = jnp.einsum('zk,kfmy->fzmy', projection_full, adjoint_block, precision=highest).astype(jnp.bfloat16).astype(jnp.float32)
        fields = jnp.einsum('xm,fzmy->fzxy', hartley_full, lifted_fields, precision=highest)
        adjoint = jnp.einsum('xm,fzmy->fzxy', hartley_full, lifted_adjoint, precision=highest)
        gradient = product_gradient(fields, adjoint).astype(jnp.float32)
        turned = jnp.einsum('xm,fzxy->fzmy', hartley_full, gradient, precision=highest).astype(jnp.bfloat16).astype(jnp.float32)
        spectral = jnp.einsum('zk,fzmy->kfmy', synthesis_full, turned, precision=highest)
        return spectral.astype(jnp.bfloat16)
    blocks = lax.map(one_block, jnp.arange(block_count, dtype=jnp.int32))
    return jnp.moveaxis(blocks, 0, 3).reshape(NZ, FIELDS, NX * Y)
```

```python
import math

import jax
import jax.numpy as jnp
from jax import lax
from jax.experimental import pallas as pl
from jax.experimental.pallas import tpu as pltpu
from jax.sharding import PartitionSpec as P

NZ = 512
MZ = 768
NX = 768
Y = 16
N = 16
XB = NX // N
MESH = pl.DeviceIdType.MESH
F32 = jnp.float32
BF16 = jnp.bfloat16
NT = (((1,), (1,)), ((), ()))
TN = (((0,), (0,)), ((), ()))


def cosine_table():
    row_index = jnp.arange(MZ, dtype=jnp.int32)
    col_index = jnp.arange(NZ, dtype=jnp.int32)
    position = col_index[None, :] * (2 * row_index[:, None] + 1) % (4 * MZ)
    return jnp.cos(jnp.pi * position.astype(jnp.float32) / (2 * MZ))


def hartley_table():
    points = jnp.arange(NX, dtype=jnp.int32)
    position = points[:, None] * points[None, :] % NX
    phases = 2.0 * jnp.pi * position.astype(jnp.float32) / NX
    return ((jnp.cos(phases) + jnp.sin(phases)) / math.sqrt(NX)).astype(jnp.bfloat16)


def iota(shape, dim):
    return lax.broadcasted_iota(jnp.int32, shape, dim)


def dot(a, b, dims=(((1,), (0,)), ((), ()))):
    return lax.dot_general(a, b, dims, preferred_element_type=F32)


def kernel(
    fm_ref, ct_ref, h_hbm, st_hbm, pt_hbm, out_ref,
    h_ref, st_ref, pt_ref, send1, recv1, send2, recv2, send3, recv3, send4, recv4,
    lift_ref, tab_sem, ssem, rsem,
):
    my_kx = lax.axis_index("kx")
    my_cz = lax.axis_index("cz")
    me = {"kx": my_kx, "cz": my_cz}

    barrier = pltpu.get_barrier_semaphore()
    for axis in ("kx", "cz"):
        for d in range(1, N):
            peer = lax.rem(me[axis] + d, N)
            pl.semaphore_signal(barrier, inc=1, device_id={axis: peer}, device_id_type=MESH)
    tables = [
        pltpu.make_async_copy(src, dst, tab_sem.at[i])
        for i, (src, dst) in enumerate(((h_hbm, h_ref), (st_hbm, st_ref), (pt_hbm, pt_ref)))
    ]
    for t in tables:
        t.start()

    def exchange(stage, axis, src, dst):
        copies = []
        for d in range(1, N):
            peer = lax.rem(me[axis] + d, N)
            c = pltpu.make_async_remote_copy(
                src_ref=src.at[peer], dst_ref=dst.at[me[axis]],
                send_sem=ssem.at[stage], recv_sem=rsem.at[stage],
                device_id={axis: peer}, device_id_type=MESH,
            )
            c.start()
        dst[me[axis]] = src[me[axis]]

    def wait_recv(stage, dst):
        pltpu.make_async_copy(dst.at[pl.ds(0, N - 1)], dst.at[pl.ds(0, N - 1)], rsem.at[stage]).wait()

    def wait_send(stage, src):
        pltpu.make_async_copy(src.at[pl.ds(0, N - 1)], src.at[pl.ds(0, N - 1)], ssem.at[stage]).wait()

    r, c = iota((128, 128), 0), iota((128, 128), 1)
    perm = (c == (r % 8) * 16 + r // 8).astype(F32).astype(BF16)
    r, c = iota((512, 512), 0), iota((512, 512), 1)
    group = (c == (r % 4) * 128 + r // 4).astype(F32).astype(BF16)

    for arr, ref in enumerate((fm_ref, ct_ref)):
        parts = []
        for j in range(6):
            block = ref[:, :, 128 * j:128 * (j + 1)].reshape(128, 128)
            parts.append(dot(perm, block, NT).reshape(16, 8, 128))
        send1[arr] = jnp.concatenate(parts, axis=1).astype(BF16)
        if arr == 0:
            pl.semaphore_wait(barrier, 2 * (N - 1))
        exchange(arr, "kx", send1.at[arr], recv1.at[arr])

    for arr in range(2):
        wait_recv(arr, recv1.at[arr])
        if arr == 0:
            tables[0].wait()
        got = recv1[arr].reshape(NX, 128)
        send2[arr] = dot(h_ref[...], got).astype(BF16).reshape(N, XB, 128)
        exchange(2 + arr, "cz", send2.at[arr], recv2.at[arr])

    tables[1].wait()
    tables[2].wait()
    for arr in range(2):
        wait_recv(2 + arr, recv2.at[arr])
        rows = jnp.concatenate(
            [jnp.concatenate([recv2[arr, 4 * g + i] for i in range(4)], axis=1) for g in range(4)],
            axis=0,
        )
        rows = dot(rows, group).astype(BF16)
        rows = jnp.concatenate(
            [
                jnp.concatenate(
                    [rows[XB * g:XB * (g + 1), 128 * f:128 * (f + 1)] for g in range(4)], axis=1)
                for f in range(4)
            ],
            axis=0,
        )
        table = (st_ref, pt_ref)[arr]
        lift_ref[arr] = dot(rows, table[...]).reshape(4, XB, MZ)

    u, v, w, b = (lift_ref[0, f] for f in range(4))
    au, av, aw, ab = (lift_ref[1, f] for f in range(4))
    grad = jnp.concatenate(
        [
            (au * w).astype(BF16),
            (av * w).astype(BF16),
            (au * u + av * v + 2.0 * aw * w + ab * b).astype(BF16),
            (ab * w).astype(BF16),
        ],
        axis=0,
    )
    back = dot(grad, st_ref[...], NT).astype(BF16)
    back = jnp.concatenate(
        [
            jnp.concatenate(
                [back[XB * f:XB * (f + 1), 128 * g:128 * (g + 1)] for f in range(4)], axis=1)
            for g in range(4)
        ],
        axis=0,
    )
    back = dot(back, group, NT).astype(BF16)
    for g in range(4):
        for i in range(4):
            send3[4 * g + i] = back[XB * g:XB * (g + 1), 128 * i:128 * (i + 1)]
    exchange(4, "cz", send3, recv3)
    wait_recv(4, recv3)
    send4[...] = dot(h_ref[...], recv3[...].reshape(NX, 128)).astype(BF16).reshape(N, XB, 128)
    exchange(5, "kx", send4, recv4)
    wait_recv(5, recv4)
    got = recv4[...].astype(F32)
    for j in range(6):
        block = got[:, 8 * j:8 * (j + 1), :].reshape(128, 128).astype(BF16)
        out_ref[:, :, 128 * j:128 * (j + 1)] = dot(block, perm, TN).astype(BF16).reshape(32, 4, 128)
    for arr in range(2):
        wait_send(arr, send1.at[arr])
        wait_send(2 + arr, send2.at[arr])
    wait_send(4, send3)
    wait_send(5, send4)


def on_device(field_modes, cotangent):
    cosines = cosine_table()
    synthesis = (cosines * math.sqrt(2.0 / NZ)).astype(BF16).T
    projection = (cosines * math.sqrt(2.0 / MZ)).astype(BF16).T
    hartley = hartley_table()
    vmem = pl.BlockSpec(memory_space=pltpu.VMEM)
    hbm = pl.BlockSpec(memory_space=pl.ANY)
    one = pltpu.VMEM((N, XB, 128), BF16)
    two = pltpu.VMEM((2, N, XB, 128), BF16)
    return pl.pallas_call(
        kernel,
        out_shape=jax.ShapeDtypeStruct(field_modes.shape, BF16),
        in_specs=[vmem, vmem, hbm, hbm, hbm],
        out_specs=vmem,
        scratch_shapes=[
            pltpu.VMEM((NX, NX), BF16),
            pltpu.VMEM((NZ, MZ), BF16),
            pltpu.VMEM((NZ, MZ), BF16),
            two, two, two, two, one, one, one, one,
            pltpu.VMEM((2, 4, XB, MZ), F32),
            pltpu.SemaphoreType.DMA((3,)),
            pltpu.SemaphoreType.DMA((6,)),
            pltpu.SemaphoreType.DMA((6,)),
        ],
        compiler_params=pltpu.CompilerParams(collective_id=0, has_side_effects=True),
    )(field_modes, cotangent, hartley, synthesis, projection)


def solution(mesh):
    return jax.shard_map(
        on_device,
        mesh=mesh,
        in_specs=(P("cz", None, "kx"), P("cz", None, "kx")),
        out_specs=P("cz", None, "kx"),
        check_vma=False,
    )
```

```python
import math

import jax
import jax.numpy as jnp
import numpy as np
from jax import lax
from jax.experimental import pallas as pl
from jax.experimental.pallas import tpu as pltpu
from jax.sharding import PartitionSpec as P

NZ = 512
MZ = 768
NX = 768
Y = 16
N = 16
XB = NX // N
MESH = pl.DeviceIdType.MESH
F32 = jnp.float32
BF16 = jnp.bfloat16
NT = (((1,), (1,)), ((), ()))
TN = (((0,), (0,)), ((), ()))


def cosine_table():
    row_index = np.arange(MZ, dtype=np.int32)
    col_index = np.arange(NZ, dtype=np.int32)
    position = col_index[None, :] * (2 * row_index[:, None] + 1) % (4 * MZ)
    return np.cos(np.pi * position / (2 * MZ)).astype(np.float32)


def hartley_table():
    points = np.arange(NX, dtype=np.int32)
    position = points[:, None] * points[None, :] % NX
    phases = 2.0 * np.pi * position / NX
    return ((np.cos(phases) + np.sin(phases)) / math.sqrt(NX)).astype(BF16)


def iota(shape, dim):
    return lax.broadcasted_iota(jnp.int32, shape, dim)


def dot(a, b, dims=(((1,), (0,)), ((), ()))):
    return lax.dot_general(a, b, dims, preferred_element_type=F32)


def kernel(
    fm_ref, ct_ref, h_hbm, st_hbm, pt_hbm, out_ref,
    h_ref, st_ref, pt_ref, send1, recv1, send2, recv2, send3, recv3, send4, recv4,
    lift_ref, tab_sem, ssem, rsem,
):
    my_kx = lax.axis_index("kx")
    my_cz = lax.axis_index("cz")
    me = {"kx": my_kx, "cz": my_cz}

    barrier = pltpu.get_barrier_semaphore()
    for axis in ("kx", "cz"):
        for d in range(1, N):
            peer = lax.rem(me[axis] + d, N)
            pl.semaphore_signal(barrier, inc=1, device_id={axis: peer}, device_id_type=MESH)
    tables = [
        pltpu.make_async_copy(src, dst, tab_sem.at[i])
        for i, (src, dst) in enumerate(((h_hbm, h_ref), (st_hbm, st_ref), (pt_hbm, pt_ref)))
    ]
    for t in tables:
        t.start()

    def exchange(stage, axis, src, dst):
        copies = []
        for d in range(1, N):
            peer = lax.rem(me[axis] + d, N)
            c = pltpu.make_async_remote_copy(
                src_ref=src.at[peer], dst_ref=dst.at[me[axis]],
                send_sem=ssem.at[stage], recv_sem=rsem.at[stage],
                device_id={axis: peer}, device_id_type=MESH,
            )
            c.start()
        dst[me[axis]] = src[me[axis]]

    def wait_recv(stage, dst):
        pltpu.make_async_copy(dst.at[pl.ds(0, N - 1)], dst.at[pl.ds(0, N - 1)], rsem.at[stage]).wait()

    def wait_send(stage, src):
        pltpu.make_async_copy(src.at[pl.ds(0, N - 1)], src.at[pl.ds(0, N - 1)], ssem.at[stage]).wait()

    r, c = iota((128, 128), 0), iota((128, 128), 1)
    perm = (c == (r % 8) * 16 + r // 8).astype(F32).astype(BF16)
    r, c = iota((512, 512), 0), iota((512, 512), 1)
    group = (c == (r % 4) * 128 + r // 4).astype(F32).astype(BF16)

    for arr, ref in enumerate((fm_ref, ct_ref)):
        parts = []
        for j in range(6):
            block = ref[:, :, 128 * j:128 * (j + 1)].reshape(128, 128)
            parts.append(dot(perm, block, NT).reshape(16, 8, 128))
        send1[arr] = jnp.concatenate(parts, axis=1).astype(BF16)
        if arr == 0:
            pl.semaphore_wait(barrier, 2 * (N - 1))
        exchange(arr, "kx", send1.at[arr], recv1.at[arr])

    for arr in range(2):
        wait_recv(arr, recv1.at[arr])
        if arr == 0:
            tables[0].wait()
        got = recv1[arr].reshape(NX, 128)
        send2[arr] = dot(h_ref[...], got).astype(BF16).reshape(N, XB, 128)
        exchange(2 + arr, "cz", send2.at[arr], recv2.at[arr])

    tables[1].wait()
    tables[2].wait()
    for arr in range(2):
        wait_recv(2 + arr, recv2.at[arr])
        rows = jnp.concatenate(
            [jnp.concatenate([recv2[arr, 4 * g + i] for i in range(4)], axis=1) for g in range(4)],
            axis=0,
        )
        rows = dot(rows, group).astype(BF16)
        rows = jnp.concatenate(
            [
                jnp.concatenate(
                    [rows[XB * g:XB * (g + 1), 128 * f:128 * (f + 1)] for g in range(4)], axis=1)
                for f in range(4)
            ],
            axis=0,
        )
        table = (st_ref, pt_ref)[arr]
        lift_ref[arr] = dot(rows, table[...]).reshape(4, XB, MZ)

    u, v, w, b = (lift_ref[0, f] for f in range(4))
    au, av, aw, ab = (lift_ref[1, f] for f in range(4))
    grad = jnp.concatenate(
        [
            (au * w).astype(BF16),
            (av * w).astype(BF16),
            (au * u + av * v + 2.0 * aw * w + ab * b).astype(BF16),
            (ab * w).astype(BF16),
        ],
        axis=0,
    )
    back = dot(grad, st_ref[...], NT).astype(BF16)
    back = jnp.concatenate(
        [
            jnp.concatenate(
                [back[XB * f:XB * (f + 1), 128 * g:128 * (g + 1)] for f in range(4)], axis=1)
            for g in range(4)
        ],
        axis=0,
    )
    back = dot(back, group, NT).astype(BF16)
    for g in range(4):
        for i in range(4):
            send3[4 * g + i] = back[XB * g:XB * (g + 1), 128 * i:128 * (i + 1)]
    exchange(4, "cz", send3, recv3)
    wait_recv(4, recv3)
    send4[...] = dot(h_ref[...], recv3[...].reshape(NX, 128)).astype(BF16).reshape(N, XB, 128)
    exchange(5, "kx", send4, recv4)
    wait_recv(5, recv4)
    got = recv4[...].astype(F32)
    for j in range(6):
        block = got[:, 8 * j:8 * (j + 1), :].reshape(128, 128).astype(BF16)
        out_ref[:, :, 128 * j:128 * (j + 1)] = dot(block, perm, TN).astype(BF16).reshape(32, 4, 128)
    for arr in range(2):
        wait_send(arr, send1.at[arr])
        wait_send(2 + arr, send2.at[arr])
    wait_send(4, send3)
    wait_send(5, send4)


def on_device(field_modes, cotangent):
    cosines = cosine_table()
    synthesis = jnp.asarray((cosines * math.sqrt(2.0 / NZ)).astype(BF16).T)
    projection = jnp.asarray((cosines * math.sqrt(2.0 / MZ)).astype(BF16).T)
    hartley = jnp.asarray(hartley_table())
    vmem = pl.BlockSpec(memory_space=pltpu.VMEM)
    hbm = pl.BlockSpec(memory_space=pl.ANY)
    one = pltpu.VMEM((N, XB, 128), BF16)
    two = pltpu.VMEM((2, N, XB, 128), BF16)
    return pl.pallas_call(
        kernel,
        out_shape=jax.ShapeDtypeStruct(field_modes.shape, BF16),
        in_specs=[vmem, vmem, hbm, hbm, hbm],
        out_specs=vmem,
        scratch_shapes=[
            pltpu.VMEM((NX, NX), BF16),
            pltpu.VMEM((NZ, MZ), BF16),
            pltpu.VMEM((NZ, MZ), BF16),
            two, two, two, two, one, one, one, one,
            pltpu.VMEM((2, 4, XB, MZ), F32),
            pltpu.SemaphoreType.DMA((3,)),
            pltpu.SemaphoreType.DMA((6,)),
            pltpu.SemaphoreType.DMA((6,)),
        ],
        compiler_params=pltpu.CompilerParams(collective_id=0, has_side_effects=True),
    )(field_modes, cotangent, hartley, synthesis, projection)


def solution(mesh):
    return jax.shard_map(
        on_device,
        mesh=mesh,
        in_specs=(P("cz", None, "kx"), P("cz", None, "kx")),
        out_specs=P("cz", None, "kx"),
        check_vma=False,
    )
```

```python
import math

import jax
import jax.numpy as jnp
import numpy as np
from jax import lax
from jax.experimental import pallas as pl
from jax.experimental.pallas import tpu as pltpu
from jax.sharding import PartitionSpec as P

NZ = 512
MZ = 768
NX = 768
Y = 16
N = 16
XB = NX // N
MESH = pl.DeviceIdType.MESH
F32 = jnp.float32
BF16 = jnp.bfloat16
NT = (((1,), (1,)), ((), ()))
TN = (((0,), (0,)), ((), ()))


def cosine_table():
    row_index = np.arange(MZ, dtype=np.int32)
    col_index = np.arange(NZ, dtype=np.int32)
    position = col_index[None, :] * (2 * row_index[:, None] + 1) % (4 * MZ)
    return np.cos(np.pi * position / (2 * MZ)).astype(np.float32)


def hartley_table():
    points = np.arange(NX, dtype=np.int32)
    position = points[:, None] * points[None, :] % NX
    phases = 2.0 * np.pi * position / NX
    return ((np.cos(phases) + np.sin(phases)) / math.sqrt(NX)).astype(BF16)


def iota(shape, dim):
    return lax.broadcasted_iota(jnp.int32, shape, dim)


def dot(a, b, dims=(((1,), (0,)), ((), ()))):
    return lax.dot_general(a, b, dims, preferred_element_type=F32)


def kernel(
    fm_hbm, ct_hbm, h_hbm, st_hbm, pt_hbm, out_ref,
    in_ref, h_ref, st_ref, pt_ref, send1, recv1, send2, recv2, send3, recv3, send4, recv4,
    lift_ref, perm_ref, group_ref, in_sem, ssem, rsem, ready, known,
):
    my_kx = lax.axis_index("kx")
    my_cz = lax.axis_index("cz")
    me = {"kx": my_kx, "cz": my_cz}
    level, side = my_kx // 2, my_kx % 2

    def signal(sem, axis, peer):
        pl.semaphore_signal(sem, inc=1, device_id={axis: peer}, device_id_type=MESH)

    barrier = pltpu.get_barrier_semaphore()
    partner = my_kx + 1 - 2 * side
    core_peer = my_cz + 1 - 2 * (my_cz % 2)
    x_peer = my_cz + 2 - 4 * (my_cz // 2 % 2)
    y_peers = (lax.rem(my_cz + 4, N), lax.rem(my_cz + 12, N))
    signal(barrier, "kx", partner)
    signal(barrier, "cz", core_peer)
    signal(barrier, "cz", x_peer)
    for peer in y_peers:
        signal(barrier, "cz", peer)
    for upper in range(4, 8):
        @pl.when(level != upper)
        def _():
            for c in range(2):
                signal(barrier, "kx", 2 * upper + c)
    loads = [
        pltpu.make_async_copy(src, dst, in_sem.at[i])
        for i, (src, dst) in enumerate((
            (fm_hbm, in_ref.at[0]), (ct_hbm, in_ref.at[1]),
            (h_hbm, h_ref), (st_hbm, st_ref), (pt_hbm, pt_ref)))
    ]
    for t in loads:
        t.start()
    r, c = iota((128, 128), 0), iota((128, 128), 1)
    perm_ref[...] = (c == (r % 8) * 16 + r // 8).astype(F32).astype(BF16)
    r, c = iota((512, 512), 0), iota((512, 512), 1)
    group_ref[...] = (c == (r % 4) * 128 + r // 4).astype(F32).astype(BF16)
    pl.semaphore_wait(barrier, jnp.where(level >= 4, 19, jnp.where(level > 0, 6, 5)))

    @pl.when(level < 3)
    def _():
        signal(barrier, "kx", my_kx + 2)

    for lower in range(4):
        @pl.when(level > lower)
        def _():
            for c in range(2):
                signal(ready.at[level], "kx", 2 * lower + c)
    for peer in y_peers:
        signal(known.at[0], "cz", peer)

    def copy(stage, axis, src, dst, peer):
        return pltpu.make_async_remote_copy(
            src_ref=src.at[peer], dst_ref=dst.at[me[axis]],
            send_sem=ssem.at[stage], recv_sem=rsem.at[stage],
            device_id={axis: peer}, device_id_type=MESH,
        )

    def exchange(stage, axis, src, dst, first=None):
        if first is not None:
            @pl.when(me[axis] != first)
            def _():
                copy(stage, axis, src, dst, first).start()
        for d in (8, 7, 9, 6, 10, 5, 11, 4, 12, 3, 13, 2, 14, 1, 15):
            peer = lax.rem(me[axis] + d, N)
            if first is None:
                copy(stage, axis, src, dst, peer).start()
            else:
                @pl.when(peer != first)
                def _():
                    copy(stage, axis, src, dst, peer).start()
        dst[me[axis]] = src[me[axis]]

    def wait_recv(stage, dst):
        pltpu.make_async_copy(dst.at[pl.ds(0, N - 1)], dst.at[pl.ds(0, N - 1)], rsem.at[stage]).wait()

    def wait_send(stage, src):
        pltpu.make_async_copy(src.at[pl.ds(0, N - 1)], src.at[pl.ds(0, N - 1)], ssem.at[stage]).wait()

    def to_level(arr, dest):
        for c in range(2):
            copy(arr, "kx", send1.at[arr], recv1.at[arr], 2 * dest + c).start()

    for arr in range(2):
        loads[arr].wait()
        parts = []
        for j in range(6):
            block = in_ref[arr, :, :, 128 * j:128 * (j + 1)].reshape(128, 128)
            parts.append(dot(perm_ref[...], block, NT).reshape(16, 8, 128))
        send1[arr] = jnp.concatenate(parts, axis=1).astype(BF16)
        for d in (4, 3, 5, 2, 6, 1, 7):
            dest = lax.rem(level + d, 8)

            @pl.when(jnp.logical_or(level >= 4, dest < level))
            def _():
                to_level(arr, dest)
        copy(arr, "kx", send1.at[arr], recv1.at[arr], partner).start()
        recv1[arr, my_kx] = send1[arr, my_kx]

    for upper in range(1, 4):
        @pl.when(level < upper)
        def _():
            pl.semaphore_wait(ready.at[upper], 2)
            for arr in range(2):
                to_level(arr, upper)

    @pl.when(level < 4)
    def _():
        uppers = [
            jnp.where(level == 0, a, jnp.where(level == 1, b, jnp.where(level == 2, c, d)))
            for a, b, c, d in ((7, 7, 4, 4), (6, 4, 5, 5), (5, 6, 7, 6), (4, 5, 6, 7))
        ]
        for upper in uppers:
            pl.semaphore_wait(ready.at[upper], 2)
            to_level(0, upper)
        for upper in uppers:
            to_level(1, upper)

    pl.semaphore_wait(known.at[0], 2)
    signal(known.at[1], "cz", x_peer)
    pl.semaphore_wait(known.at[1], 1)
    signal(known.at[2], "cz", core_peer)
    pl.semaphore_wait(known.at[2], 1)

    for arr in range(2):
        if arr == 0:
            loads[2].wait()
        wait_recv(arr, recv1.at[arr])
        got = recv1[arr].reshape(NX, 128)
        send2[arr] = dot(h_ref[...], got).astype(BF16).reshape(N, XB, 128)
        exchange(2 + arr, "cz", send2.at[arr], recv2.at[arr])

    loads[3].wait()
    loads[4].wait()
    for arr in range(2):
        wait_recv(2 + arr, recv2.at[arr])
        rows = jnp.concatenate(
            [jnp.concatenate([recv2[arr, 4 * g + i] for i in range(4)], axis=1) for g in range(4)],
            axis=0,
        )
        rows = dot(rows, group_ref[...]).astype(BF16)
        rows = jnp.concatenate(
            [
                jnp.concatenate(
                    [rows[XB * g:XB * (g + 1), 128 * f:128 * (f + 1)] for g in range(4)], axis=1)
                for f in range(4)
            ],
            axis=0,
        )
        table = (st_ref, pt_ref)[arr]
        lift_ref[arr] = dot(rows, table[...]).reshape(4, XB, MZ)

    u, v, w, b = (lift_ref[0, f] for f in range(4))
    au, av, aw, ab = (lift_ref[1, f] for f in range(4))
    grad = jnp.concatenate(
        [
            (au * w).astype(BF16),
            (av * w).astype(BF16),
            (au * u + av * v + 2.0 * aw * w + ab * b).astype(BF16),
            (ab * w).astype(BF16),
        ],
        axis=0,
    )
    back = dot(grad, st_ref[...], NT).astype(BF16)
    back = jnp.concatenate(
        [
            jnp.concatenate(
                [back[XB * f:XB * (f + 1), 128 * g:128 * (g + 1)] for f in range(4)], axis=1)
            for g in range(4)
        ],
        axis=0,
    )
    back = dot(back, group_ref[...], NT).astype(BF16)
    for g in range(4):
        for i in range(4):
            send3[4 * g + i] = back[XB * g:XB * (g + 1), 128 * i:128 * (i + 1)]
    exchange(4, "cz", send3, recv3)
    wait_recv(4, recv3)
    send4[...] = dot(h_ref[...], recv3[...].reshape(NX, 128)).astype(BF16).reshape(N, XB, 128)
    exchange(5, "kx", send4, recv4, first=0)
    wait_recv(5, recv4)
    out_ref[...] = recv4[...]
    for arr in range(2):
        wait_send(arr, send1.at[arr])
        wait_send(2 + arr, send2.at[arr])
    wait_send(4, send3)
    wait_send(5, send4)


def unpack(in_ref, out_ref):
    r, c = iota((128, 128), 0), iota((128, 128), 1)
    perm = (c == (r % 8) * 16 + r // 8).astype(F32).astype(BF16)
    got = in_ref[...].astype(F32)
    for j in range(6):
        block = got[:, 8 * j:8 * (j + 1), :].reshape(128, 128).astype(BF16)
        out_ref[:, :, 128 * j:128 * (j + 1)] = dot(block, perm, TN).astype(BF16).reshape(32, 4, 128)


def on_device(field_modes, cotangent):
    cosines = cosine_table()
    synthesis = jnp.asarray((cosines * math.sqrt(2.0 / NZ)).astype(BF16).T)
    projection = jnp.asarray((cosines * math.sqrt(2.0 / MZ)).astype(BF16).T)
    hartley = jnp.asarray(hartley_table())
    vmem = pl.BlockSpec(memory_space=pltpu.VMEM)
    hbm = pl.BlockSpec(memory_space=pl.ANY)
    one = pltpu.VMEM((N, XB, 128), BF16)
    two = pltpu.VMEM((2, N, XB, 128), BF16)
    blocks = pl.pallas_call(
        kernel,
        out_shape=pltpu.VMEM((N, XB, 128), BF16),
        in_specs=[hbm] * 5,
        out_specs=vmem,
        scratch_shapes=[
            pltpu.VMEM((2,) + field_modes.shape, BF16),
            pltpu.VMEM((NX, NX), BF16),
            pltpu.VMEM((NZ, MZ), BF16),
            pltpu.VMEM((NZ, MZ), BF16),
            two, two, two, two, one, one, one, one,
            pltpu.VMEM((2, 4, XB, MZ), F32),
            pltpu.VMEM((128, 128), BF16),
            pltpu.VMEM((512, 512), BF16),
            pltpu.SemaphoreType.DMA((5,)),
            pltpu.SemaphoreType.DMA((6,)),
            pltpu.SemaphoreType.DMA((6,)),
            pltpu.SemaphoreType.REGULAR((8,)),
            pltpu.SemaphoreType.REGULAR((3,)),
        ],
        compiler_params=pltpu.CompilerParams(collective_id=0, has_side_effects=True),
    )(field_modes, cotangent, hartley, synthesis, projection)
    return pl.pallas_call(
        unpack,
        out_shape=jax.ShapeDtypeStruct(field_modes.shape, BF16),
        in_specs=[vmem],
        out_specs=vmem,
    )(pltpu.with_memory_space_constraint(blocks, pltpu.VMEM))


def solution(mesh):
    return jax.shard_map(
        on_device,
        mesh=mesh,
        in_specs=(P("cz", None, "kx"), P("cz", None, "kx")),
        out_specs=P("cz", None, "kx"),
        check_vma=False,
    )
```

```python
import math

import jax
import jax.numpy as jnp
import numpy as np
from jax import lax
from jax.experimental import pallas as pl
from jax.experimental.pallas import tpu as pltpu
from jax.sharding import PartitionSpec as P

NZ = 512
MZ = 768
NX = 768
Y = 16
N = 16
XB = NX // N
MESH = pl.DeviceIdType.MESH
F32 = jnp.float32
BF16 = jnp.bfloat16
NT = (((1,), (1,)), ((), ()))
TN = (((0,), (0,)), ((), ()))


def cosine_table():
    row_index = np.arange(MZ, dtype=np.int32)
    col_index = np.arange(NZ, dtype=np.int32)
    position = col_index[None, :] * (2 * row_index[:, None] + 1) % (4 * MZ)
    return np.cos(np.pi * position / (2 * MZ)).astype(np.float32)


def hartley_table():
    points = np.arange(NX, dtype=np.int32)
    position = points[:, None] * points[None, :] % NX
    phases = 2.0 * np.pi * position / NX
    return ((np.cos(phases) + np.sin(phases)) / math.sqrt(NX)).astype(BF16)


def iota(shape, dim):
    return lax.broadcasted_iota(jnp.int32, shape, dim)


def dot(a, b, dims=(((1,), (0,)), ((), ()))):
    return lax.dot_general(a, b, dims, preferred_element_type=F32)


def kernel(
    fm_hbm, ct_hbm, h_hbm, st_hbm, pt_hbm, out_ref,
    in_ref, h_ref, st_ref, pt_ref, send1, recv1, send2, recv2, send3, recv3, send4, recv4,
    lift_ref, perm_ref, group_ref, in_sem, ssem, rsem, ready, known, chain,
):
    my_kx = lax.axis_index("kx")
    my_cz = lax.axis_index("cz")
    me = {"kx": my_kx, "cz": my_cz}
    level, side = my_kx // 2, my_kx % 2

    def signal(sem, axis, peer):
        pl.semaphore_signal(sem, inc=1, device_id={axis: peer}, device_id_type=MESH)

    barrier = pltpu.get_barrier_semaphore()
    partner = my_kx + 1 - 2 * side
    core_peer = my_cz + 1 - 2 * (my_cz % 2)
    x_peer = my_cz + 2 - 4 * (my_cz // 2 % 2)
    y_peers = (lax.rem(my_cz + 4, N), lax.rem(my_cz + 12, N))
    signal(barrier, "kx", partner)
    signal(barrier, "cz", core_peer)
    signal(barrier, "cz", x_peer)
    for peer in y_peers:
        signal(barrier, "cz", peer)
    for upper in range(4, 8):
        near = jnp.logical_or(level == upper - 1, level == upper + 1)

        @pl.when(jnp.logical_or(level < 4, near))
        def _():
            for c in range(2):
                signal(barrier, "kx", 2 * upper + c)
    loads = [
        pltpu.make_async_copy(src, dst, in_sem.at[i])
        for i, (src, dst) in enumerate((
            (fm_hbm, in_ref.at[0]), (ct_hbm, in_ref.at[1]),
            (h_hbm, h_ref), (st_hbm, st_ref), (pt_hbm, pt_ref)))
    ]
    for t in loads:
        t.start()
    r, c = iota((128, 128), 0), iota((128, 128), 1)
    perm_ref[...] = (c == (r % 8) * 16 + r // 8).astype(F32).astype(BF16)
    r, c = iota((512, 512), 0), iota((512, 512), 1)
    group_ref[...] = (c == (r % 4) * 128 + r // 4).astype(F32).astype(BF16)
    ends = jnp.logical_or(level == 4, level == 7)
    middle = jnp.logical_or(level == 5, level == 6)
    entered = jnp.where(ends, 15, jnp.where(middle, 17, jnp.where(level > 0, 6, 5)))
    pl.semaphore_wait(barrier, entered)

    @pl.when(level < 3)
    def _():
        signal(barrier, "kx", my_kx + 2)

    for lower in range(4):
        @pl.when(level > lower)
        def _():
            for c in range(2):
                signal(ready.at[level], "kx", 2 * lower + c)
    @pl.when(middle)
    def _():
        signal(chain.at[0], "kx", my_kx + 2)
        signal(chain.at[1], "kx", my_kx - 2)

    for peer in y_peers:
        signal(known.at[0], "cz", peer)

    def copy(stage, axis, src, dst, peer):
        return pltpu.make_async_remote_copy(
            src_ref=src.at[peer], dst_ref=dst.at[me[axis]],
            send_sem=ssem.at[stage], recv_sem=rsem.at[stage],
            device_id={axis: peer}, device_id_type=MESH,
        )

    def exchange(stage, axis, src, dst, by_index=False):
        if by_index:
            for peer in range(N):
                @pl.when(me[axis] != peer)
                def _():
                    copy(stage, axis, src, dst, peer).start()
        else:
            for d in (8, 7, 9, 6, 10, 5, 11, 4, 12, 3, 13, 2, 14, 1, 15):
                copy(stage, axis, src, dst, lax.rem(me[axis] + d, N)).start()
        dst[me[axis]] = src[me[axis]]

    def wait_recv(stage, dst):
        pltpu.make_async_copy(dst.at[pl.ds(0, N - 1)], dst.at[pl.ds(0, N - 1)], rsem.at[stage]).wait()

    def wait_send(stage, src):
        pltpu.make_async_copy(src.at[pl.ds(0, N - 1)], src.at[pl.ds(0, N - 1)], ssem.at[stage]).wait()

    def to_level(arr, dest):
        for c in range(2):
            copy(arr, "kx", send1.at[arr], recv1.at[arr], 2 * dest + c).start()

    def prepare(arr):
        loads[arr].wait()
        parts = []
        for j in range(6):
            block = in_ref[arr, :, :, 128 * j:128 * (j + 1)].reshape(128, 128)
            parts.append(dot(perm_ref[...], block, NT).reshape(16, 8, 128))
        send1[arr] = jnp.concatenate(parts, axis=1).astype(BF16)

    def to_levels(arr, allowed):
        for d in (4, 3, 5, 2, 6, 1, 7):
            dest = lax.rem(level + d, 8)

            @pl.when(allowed(dest, d))
            def _():
                to_level(arr, dest)

    def to_partner(arr):
        copy(arr, "kx", send1.at[arr], recv1.at[arr], partner).start()
        recv1[arr, my_kx] = send1[arr, my_kx]

    def lower_ones(dest, d):
        low = jnp.logical_and(dest < 4, jnp.logical_or(level >= 4, dest < level))
        return jnp.logical_or(low, jnp.logical_and(level >= 4, dest >= 4)) if d in (1, 7) else low

    prepare(0)
    to_levels(0, lower_ones)
    to_partner(0)
    prepare(1)

    @pl.when(level == 5)
    def _():
        pl.semaphore_wait(chain.at[1], 1)
        signal(chain.at[3], "kx", my_kx - 2)
        to_level(0, 7)

    @pl.when(level == 6)
    def _():
        pl.semaphore_wait(chain.at[0], 1)
        signal(chain.at[2], "kx", my_kx + 2)
        to_level(0, 4)

    @pl.when(level == 4)
    def _():
        pl.semaphore_wait(chain.at[1], 1)
        to_level(0, 6)
        pl.semaphore_wait(chain.at[3], 1)
        to_level(0, 7)

    @pl.when(level == 7)
    def _():
        pl.semaphore_wait(chain.at[0], 1)
        to_level(0, 5)
        pl.semaphore_wait(chain.at[2], 1)
        to_level(0, 4)

    to_levels(1, lambda dest, d: jnp.logical_or(level >= 4, dest < level))
    to_partner(1)

    for upper in range(1, 4):
        @pl.when(level < upper)
        def _():
            pl.semaphore_wait(ready.at[upper], 2)
            for arr in range(2):
                to_level(arr, upper)

    @pl.when(level < 4)
    def _():
        uppers = [
            jnp.where(level == 0, a, jnp.where(level == 1, b, jnp.where(level == 2, c, d)))
            for a, b, c, d in ((7, 7, 4, 4), (6, 4, 5, 5), (5, 6, 7, 6), (4, 5, 6, 7))
        ]
        for upper in uppers:
            pl.semaphore_wait(ready.at[upper], 2)
            to_level(0, upper)
        for upper in [
            jnp.where(level == 0, a, jnp.where(level == 1, b, jnp.where(level == 2, c, d)))
            for a, b, c, d in ((5, 6, 5, 6), (6, 5, 6, 5), (7, 7, 4, 4), (4, 4, 7, 7))
        ]:
            to_level(1, upper)

    pl.semaphore_wait(known.at[0], 2)
    signal(known.at[1], "cz", x_peer)
    pl.semaphore_wait(known.at[1], 1)
    signal(known.at[2], "cz", core_peer)
    pl.semaphore_wait(known.at[2], 1)

    for arr in range(2):
        if arr == 0:
            loads[2].wait()
        wait_recv(arr, recv1.at[arr])
        got = recv1[arr].reshape(NX, 128)
        send2[arr] = dot(h_ref[...], got).astype(BF16).reshape(N, XB, 128)
        exchange(2 + arr, "cz", send2.at[arr], recv2.at[arr])

    loads[3].wait()
    loads[4].wait()
    for arr in range(2):
        wait_recv(2 + arr, recv2.at[arr])
        rows = jnp.concatenate(
            [jnp.concatenate([recv2[arr, 4 * g + i] for i in range(4)], axis=1) for g in range(4)],
            axis=0,
        )
        rows = dot(rows, group_ref[...]).astype(BF16)
        rows = jnp.concatenate(
            [
                jnp.concatenate(
                    [rows[XB * g:XB * (g + 1), 128 * f:128 * (f + 1)] for g in range(4)], axis=1)
                for f in range(4)
            ],
            axis=0,
        )
        table = (st_ref, pt_ref)[arr]
        lift_ref[arr] = dot(rows, table[...]).reshape(4, XB, MZ)

    u, v, w, b = (lift_ref[0, f] for f in range(4))
    au, av, aw, ab = (lift_ref[1, f] for f in range(4))
    grad = jnp.concatenate(
        [
            (au * w).astype(BF16),
            (av * w).astype(BF16),
            (au * u + av * v + 2.0 * aw * w + ab * b).astype(BF16),
            (ab * w).astype(BF16),
        ],
        axis=0,
    )
    back = dot(grad, st_ref[...], NT).astype(BF16)
    back = jnp.concatenate(
        [
            jnp.concatenate(
                [back[XB * f:XB * (f + 1), 128 * g:128 * (g + 1)] for f in range(4)], axis=1)
            for g in range(4)
        ],
        axis=0,
    )
    back = dot(back, group_ref[...], NT).astype(BF16)
    for g in range(4):
        for i in range(4):
            send3[4 * g + i] = back[XB * g:XB * (g + 1), 128 * i:128 * (i + 1)]
    exchange(4, "cz", send3, recv3)
    wait_recv(4, recv3)
    send4[...] = dot(h_ref[...], recv3[...].reshape(NX, 128)).astype(BF16).reshape(N, XB, 128)
    exchange(5, "kx", send4, recv4, by_index=True)
    wait_recv(5, recv4)
    out_ref[...] = recv4[...]
    for arr in range(2):
        wait_send(arr, send1.at[arr])
        wait_send(2 + arr, send2.at[arr])
    wait_send(4, send3)
    wait_send(5, send4)


def unpack(in_ref, out_ref):
    r, c = iota((128, 128), 0), iota((128, 128), 1)
    perm = (c == (r % 8) * 16 + r // 8).astype(F32).astype(BF16)
    got = in_ref[...].astype(F32)
    for j in range(6):
        block = got[:, 8 * j:8 * (j + 1), :].reshape(128, 128).astype(BF16)
        out_ref[:, :, 128 * j:128 * (j + 1)] = dot(block, perm, TN).astype(BF16).reshape(32, 4, 128)


def on_device(field_modes, cotangent):
    cosines = cosine_table()
    synthesis = jnp.asarray((cosines * math.sqrt(2.0 / NZ)).astype(BF16).T)
    projection = jnp.asarray((cosines * math.sqrt(2.0 / MZ)).astype(BF16).T)
    hartley = jnp.asarray(hartley_table())
    vmem = pl.BlockSpec(memory_space=pltpu.VMEM)
    hbm = pl.BlockSpec(memory_space=pl.ANY)
    one = pltpu.VMEM((N, XB, 128), BF16)
    two = pltpu.VMEM((2, N, XB, 128), BF16)
    blocks = pl.pallas_call(
        kernel,
        out_shape=pltpu.VMEM((N, XB, 128), BF16),
        in_specs=[hbm] * 5,
        out_specs=vmem,
        scratch_shapes=[
            pltpu.VMEM((2,) + field_modes.shape, BF16),
            pltpu.VMEM((NX, NX), BF16),
            pltpu.VMEM((NZ, MZ), BF16),
            pltpu.VMEM((NZ, MZ), BF16),
            two, two, two, two, one, one, one, one,
            pltpu.VMEM((2, 4, XB, MZ), F32),
            pltpu.VMEM((128, 128), BF16),
            pltpu.VMEM((512, 512), BF16),
            pltpu.SemaphoreType.DMA((5,)),
            pltpu.SemaphoreType.DMA((6,)),
            pltpu.SemaphoreType.DMA((6,)),
            pltpu.SemaphoreType.REGULAR((8,)),
            pltpu.SemaphoreType.REGULAR((3,)),
            pltpu.SemaphoreType.REGULAR((4,)),
        ],
        compiler_params=pltpu.CompilerParams(collective_id=0, has_side_effects=True),
    )(field_modes, cotangent, hartley, synthesis, projection)
    return pl.pallas_call(
        unpack,
        out_shape=jax.ShapeDtypeStruct(field_modes.shape, BF16),
        in_specs=[vmem],
        out_specs=vmem,
    )(pltpu.with_memory_space_constraint(blocks, pltpu.VMEM))


def solution(mesh):
    return jax.shard_map(
        on_device,
        mesh=mesh,
        in_specs=(P("cz", None, "kx"), P("cz", None, "kx")),
        out_specs=P("cz", None, "kx"),
        check_vma=False,
    )
```

```python
import math

import jax
import jax.numpy as jnp
import numpy as np
from jax import lax
from jax.experimental import pallas as pl
from jax.experimental.pallas import tpu as pltpu
from jax.sharding import PartitionSpec as P

NZ = 512
MZ = 768
NX = 768
Y = 16
N = 16
XB = NX // N
PARTS = 4
MESH = pl.DeviceIdType.MESH
F32 = jnp.float32
BF16 = jnp.bfloat16
NT = (((1,), (1,)), ((), ()))
TN = (((0,), (0,)), ((), ()))


def cosine_table():
    row_index = np.arange(MZ, dtype=np.int32)
    col_index = np.arange(NZ, dtype=np.int32)
    position = col_index[None, :] * (2 * row_index[:, None] + 1) % (4 * MZ)
    return np.cos(np.pi * position / (2 * MZ)).astype(np.float32)


def hartley_table():
    points = np.arange(NX, dtype=np.int32)
    position = points[:, None] * points[None, :] % NX
    phases = 2.0 * np.pi * position / NX
    return ((np.cos(phases) + np.sin(phases)) / math.sqrt(NX)).astype(BF16)


def iota(shape, dim):
    return lax.broadcasted_iota(jnp.int32, shape, dim)


def dot(a, b, dims=(((1,), (0,)), ((), ()))):
    return lax.dot_general(a, b, dims, preferred_element_type=F32)


def kernel(
    fm_hbm, ct_hbm, h_hbm, st_hbm, pt_hbm, out_ref,
    in_ref, h_ref, st_ref, pt_ref, send1, recv1, send2, recv2, send3, recv3, send4, recv4,
    lift_ref, perm_ref, group_ref, in_sem, ssem, rsem, ready, known, chain,
):
    my_kx = lax.axis_index("kx")
    my_cz = lax.axis_index("cz")
    me = {"kx": my_kx, "cz": my_cz}
    level, side = my_kx // 2, my_kx % 2

    def signal(sem, axis, peer):
        pl.semaphore_signal(sem, inc=1, device_id={axis: peer}, device_id_type=MESH)

    barrier = pltpu.get_barrier_semaphore()
    partner = my_kx + 1 - 2 * side
    core_peer = my_cz + 1 - 2 * (my_cz % 2)
    x_peer = my_cz + 2 - 4 * (my_cz // 2 % 2)
    y_peers = (lax.rem(my_cz + 4, N), lax.rem(my_cz + 12, N))
    signal(barrier, "kx", partner)
    signal(barrier, "cz", core_peer)
    signal(barrier, "cz", x_peer)
    for peer in y_peers:
        signal(barrier, "cz", peer)
    for upper in range(4, 8):
        near = jnp.logical_or(level == upper - 1, level == upper + 1)

        @pl.when(jnp.logical_or(level < 4, near))
        def _():
            for c in range(2):
                signal(barrier, "kx", 2 * upper + c)
    loads = [
        pltpu.make_async_copy(src, dst, in_sem.at[i])
        for i, (src, dst) in enumerate((
            (fm_hbm, in_ref.at[0]), (ct_hbm, in_ref.at[1]),
            (h_hbm, h_ref), (st_hbm, st_ref), (pt_hbm, pt_ref)))
    ]
    for t in loads:
        t.start()
    r, c = iota((128, 128), 0), iota((128, 128), 1)
    perm_ref[...] = (c == (r % 8) * 16 + r // 8).astype(F32).astype(BF16)
    r, c = iota((512, 512), 0), iota((512, 512), 1)
    group_ref[...] = (c == (r % 4) * 128 + r // 4).astype(F32).astype(BF16)
    ends = jnp.logical_or(level == 4, level == 7)
    middle = jnp.logical_or(level == 5, level == 6)
    entered = jnp.where(ends, 15, jnp.where(middle, 17, jnp.where(level > 0, 6, 5)))
    pl.semaphore_wait(barrier, entered)

    @pl.when(level < 3)
    def _():
        signal(barrier, "kx", my_kx + 2)

    for lower in range(4):
        @pl.when(level > lower)
        def _():
            for c in range(2):
                signal(ready.at[level], "kx", 2 * lower + c)
    @pl.when(middle)
    def _():
        signal(chain.at[0], "kx", my_kx + 2)
        signal(chain.at[1], "kx", my_kx - 2)

    for peer in y_peers:
        signal(known.at[0], "cz", peer)

    def copy(stage, axis, src, dst, peer):
        return pltpu.make_async_remote_copy(
            src_ref=src.at[peer], dst_ref=dst.at[me[axis]],
            send_sem=ssem.at[stage], recv_sem=rsem.at[stage],
            device_id={axis: peer}, device_id_type=MESH,
        )

    def flipped(index, bits):
        for bit in (1, 2, 4, 8):
            if bits & bit:
                index = index + bit - 2 * bit * (index // bit % 2)
        return index

    def exchange(stage, axis, src, dst, by_index=False):
        if by_index:
            for peer in range(N):
                @pl.when(me[axis] != peer)
                def _():
                    copy(stage, axis, src, dst, peer).start()
        else:
            flip = {0: me[axis]}
            for d in range(1, N):
                low = d & -d
                flip[d] = flipped(flip[d - low], low)
            for d in (10, 11, 14, 15, 6, 7, 8, 9, 2, 3, 12, 13, 4, 5, 1):
                copy(stage, axis, src, dst, flip[d]).start()
        dst[me[axis]] = src[me[axis]]

    def wait_recv(stage, dst):
        pltpu.make_async_copy(dst.at[pl.ds(0, N - 1)], dst.at[pl.ds(0, N - 1)], rsem.at[stage]).wait()

    def wait_send(stage, src):
        pltpu.make_async_copy(src.at[pl.ds(0, N - 1)], src.at[pl.ds(0, N - 1)], ssem.at[stage]).wait()

    def to_level(arr, dest):
        for c in range(2):
            copy(arr, "kx", send1.at[arr], recv1.at[arr], 2 * dest + c).start()

    def prepare(arr):
        loads[arr].wait()
        parts = []
        for j in range(6):
            block = in_ref[arr, :, :, 128 * j:128 * (j + 1)].reshape(128, 128)
            parts.append(dot(perm_ref[...], block, NT).reshape(16, 8, 128))
        send1[arr] = jnp.concatenate(parts, axis=1).astype(BF16)

    def to_levels(arr, allowed):
        for d in (4, 3, 5, 2, 6, 1, 7):
            dest = lax.rem(level + d, 8)

            @pl.when(allowed(dest, d))
            def _():
                to_level(arr, dest)

    def to_partner(arr):
        copy(arr, "kx", send1.at[arr], recv1.at[arr], partner).start()
        recv1[arr, my_kx] = send1[arr, my_kx]

    def lower_ones(dest, d):
        low = jnp.logical_and(dest < 4, jnp.logical_or(level >= 4, dest < level))
        return jnp.logical_or(low, jnp.logical_and(level >= 4, dest >= 4)) if d in (1, 7) else low

    prepare(0)
    to_levels(0, lower_ones)
    to_partner(0)
    prepare(1)

    @pl.when(level == 5)
    def _():
        pl.semaphore_wait(chain.at[1], 1)
        signal(chain.at[3], "kx", my_kx - 2)
        to_level(0, 7)

    @pl.when(level == 6)
    def _():
        pl.semaphore_wait(chain.at[0], 1)
        signal(chain.at[2], "kx", my_kx + 2)
        to_level(0, 4)

    @pl.when(level == 4)
    def _():
        pl.semaphore_wait(chain.at[1], 1)
        to_level(0, 6)
        pl.semaphore_wait(chain.at[3], 1)
        to_level(0, 7)

    @pl.when(level == 7)
    def _():
        pl.semaphore_wait(chain.at[0], 1)
        to_level(0, 5)
        pl.semaphore_wait(chain.at[2], 1)
        to_level(0, 4)

    def rest_of_b():
        to_levels(1, lambda dest, d: level >= 4)

        @pl.when(level < 4)
        def _():
            for upper in range(1, 4):
                @pl.when(level < upper)
                def _():
                    to_level(1, upper)
            for upper in [
                jnp.where(level == 0, a, jnp.where(level == 1, b, jnp.where(level == 2, c, d)))
                for a, b, c, d in ((5, 6, 5, 6), (6, 5, 6, 5), (7, 7, 4, 4), (4, 4, 7, 7))
            ]:
                to_level(1, upper)
        to_partner(1)

    to_levels(1, lambda dest, d: jnp.logical_and(level < 4, dest < level))
    for upper in range(1, 4):
        @pl.when(level < upper)
        def _():
            pl.semaphore_wait(ready.at[upper], 2)
            to_level(0, upper)

    @pl.when(level < 4)
    def _():
        uppers = [
            jnp.where(level == 0, a, jnp.where(level == 1, b, jnp.where(level == 2, c, d)))
            for a, b, c, d in ((7, 7, 4, 4), (6, 4, 5, 5), (5, 6, 7, 6), (4, 5, 6, 7))
        ]
        for upper in uppers:
            pl.semaphore_wait(ready.at[upper], 2)
            to_level(0, upper)

    @pl.when(my_cz % 2 == 0)
    def _():
        rest_of_b()
    pl.semaphore_wait(known.at[0], 2)
    signal(known.at[1], "cz", x_peer)
    pl.semaphore_wait(known.at[1], 1)
    signal(known.at[2], "cz", core_peer)
    pl.semaphore_wait(known.at[2], 1)

    def transformed(i, got):
        rows = NX // PARTS
        return dot(h_ref[rows * i:rows * (i + 1)], got).astype(BF16).reshape(N // PARTS, XB, 128)

    for arr in range(2):
        if arr == 0:
            loads[2].wait()
        wait_recv(arr, recv1.at[arr])
        got = recv1[arr].reshape(NX, 128)
        for i in range(PARTS):
            send2[arr, 8 // PARTS * 2 * i:8 // PARTS * 2 * (i + 1)] = transformed(i, got)
        exchange(2 + arr, "cz", send2.at[arr], recv2.at[arr])
        if arr == 0:
            @pl.when(my_cz % 2 == 1)
            def _():
                rest_of_b()

    loads[3].wait()
    loads[4].wait()
    for arr in range(2):
        wait_recv(2 + arr, recv2.at[arr])
        rows = jnp.concatenate(
            [jnp.concatenate([recv2[arr, 4 * g + i] for i in range(4)], axis=1) for g in range(4)],
            axis=0,
        )
        rows = dot(rows, group_ref[...]).astype(BF16)
        rows = jnp.concatenate(
            [
                jnp.concatenate(
                    [rows[XB * g:XB * (g + 1), 128 * f:128 * (f + 1)] for g in range(4)], axis=1)
                for f in range(4)
            ],
            axis=0,
        )
        table = (st_ref, pt_ref)[arr]
        lift_ref[arr] = dot(rows, table[...]).reshape(4, XB, MZ)

    u, v, w, b = (lift_ref[0, f] for f in range(4))
    au, av, aw, ab = (lift_ref[1, f] for f in range(4))
    grad = jnp.concatenate(
        [
            (au * w).astype(BF16),
            (av * w).astype(BF16),
            (au * u + av * v + 2.0 * aw * w + ab * b).astype(BF16),
            (ab * w).astype(BF16),
        ],
        axis=0,
    )
    back = dot(grad, st_ref[...], NT).astype(BF16)
    back = jnp.concatenate(
        [
            jnp.concatenate(
                [back[XB * f:XB * (f + 1), 128 * g:128 * (g + 1)] for f in range(4)], axis=1)
            for g in range(4)
        ],
        axis=0,
    )
    back = dot(back, group_ref[...], NT).astype(BF16)
    for g in range(4):
        for i in range(4):
            send3[4 * g + i] = back[XB * g:XB * (g + 1), 128 * i:128 * (i + 1)]
    exchange(4, "cz", send3, recv3)
    wait_recv(4, recv3)
    got = recv3[...].reshape(NX, 128)
    for i in range(PARTS):
        send4[8 // PARTS * 2 * i:8 // PARTS * 2 * (i + 1)] = transformed(i, got)
    exchange(5, "kx", send4, recv4, by_index=True)
    wait_recv(5, recv4)
    out_ref[...] = recv4[...]
    for arr in range(2):
        wait_send(arr, send1.at[arr])
        wait_send(2 + arr, send2.at[arr])
    wait_send(4, send3)
    wait_send(5, send4)


def unpack(in_ref, out_ref):
    r, c = iota((128, 128), 0), iota((128, 128), 1)
    perm = (c == (r % 8) * 16 + r // 8).astype(F32).astype(BF16)
    got = in_ref[...].astype(F32)
    for j in range(6):
        block = got[:, 8 * j:8 * (j + 1), :].reshape(128, 128).astype(BF16)
        out_ref[:, :, 128 * j:128 * (j + 1)] = dot(block, perm, TN).astype(BF16).reshape(32, 4, 128)


def on_device(field_modes, cotangent):
    cosines = cosine_table()
    synthesis = jnp.asarray((cosines * math.sqrt(2.0 / NZ)).astype(BF16).T)
    projection = jnp.asarray((cosines * math.sqrt(2.0 / MZ)).astype(BF16).T)
    hartley = jnp.asarray(hartley_table())
    vmem = pl.BlockSpec(memory_space=pltpu.VMEM)
    hbm = pl.BlockSpec(memory_space=pl.ANY)
    one = pltpu.VMEM((N, XB, 128), BF16)
    two = pltpu.VMEM((2, N, XB, 128), BF16)
    blocks = pl.pallas_call(
        kernel,
        out_shape=pltpu.VMEM((N, XB, 128), BF16),
        in_specs=[hbm] * 5,
        out_specs=vmem,
        scratch_shapes=[
            pltpu.VMEM((2,) + field_modes.shape, BF16),
            pltpu.VMEM((NX, NX), BF16),
            pltpu.VMEM((NZ, MZ), BF16),
            pltpu.VMEM((NZ, MZ), BF16),
            two, two, two, two, one, one, one, one,
            pltpu.VMEM((2, 4, XB, MZ), F32),
            pltpu.VMEM((128, 128), BF16),
            pltpu.VMEM((512, 512), BF16),
            pltpu.SemaphoreType.DMA((5,)),
            pltpu.SemaphoreType.DMA((6,)),
            pltpu.SemaphoreType.DMA((6,)),
            pltpu.SemaphoreType.REGULAR((8,)),
            pltpu.SemaphoreType.REGULAR((3,)),
            pltpu.SemaphoreType.REGULAR((4,)),
        ],
        compiler_params=pltpu.CompilerParams(collective_id=0, has_side_effects=True),
    )(field_modes, cotangent, hartley, synthesis, projection)
    return pl.pallas_call(
        unpack,
        out_shape=jax.ShapeDtypeStruct(field_modes.shape, BF16),
        in_specs=[vmem],
        out_specs=vmem,
    )(pltpu.with_memory_space_constraint(blocks, pltpu.VMEM))


def solution(mesh):
    return jax.shard_map(
        on_device,
        mesh=mesh,
        in_specs=(P("cz", None, "kx"), P("cz", None, "kx")),
        out_specs=P("cz", None, "kx"),
        check_vma=False,
    )
```

```python
import math

import jax
import jax.numpy as jnp
import numpy as np
from jax import lax
from jax.experimental import pallas as pl
from jax.experimental.pallas import tpu as pltpu
from jax.sharding import PartitionSpec as P

NZ = 512
MZ = 768
NX = 768
Y = 16
N = 16
XB = NX // N
PARTS = 4
MESH = pl.DeviceIdType.MESH
F32 = jnp.float32
BF16 = jnp.bfloat16
NT = (((1,), (1,)), ((), ()))
TN = (((0,), (0,)), ((), ()))


def cosine_table():
    row_index = np.arange(MZ, dtype=np.int32)
    col_index = np.arange(NZ, dtype=np.int32)
    position = col_index[None, :] * (2 * row_index[:, None] + 1) % (4 * MZ)
    return np.cos(np.pi * position / (2 * MZ)).astype(np.float32)


def hartley_table():
    points = np.arange(NX, dtype=np.int32)
    position = points[:, None] * points[None, :] % NX
    phases = 2.0 * np.pi * position / NX
    return ((np.cos(phases) + np.sin(phases)) / math.sqrt(NX)).astype(BF16)


def iota(shape, dim):
    return lax.broadcasted_iota(jnp.int32, shape, dim)


def dot(a, b, dims=(((1,), (0,)), ((), ()))):
    return lax.dot_general(a, b, dims, preferred_element_type=F32)


def kernel(
    fm_hbm, ct_hbm, h_hbm, st_hbm, pt_hbm, out_ref,
    in_ref, h_ref, st_ref, pt_ref, send1, recv1, send2, recv2, send3, recv3, send4, recv4,
    lift_ref, perm_ref, group_ref, in_sem, ssem, rsem, ready, known, chain,
):
    my_kx = lax.axis_index("kx")
    my_cz = lax.axis_index("cz")
    me = {"kx": my_kx, "cz": my_cz}
    level, side = my_kx // 2, my_kx % 2

    def signal(sem, axis, peer):
        pl.semaphore_signal(sem, inc=1, device_id={axis: peer}, device_id_type=MESH)

    barrier = pltpu.get_barrier_semaphore()
    partner = my_kx + 1 - 2 * side
    core_peer = my_cz + 1 - 2 * (my_cz % 2)
    x_peer = my_cz + 2 - 4 * (my_cz // 2 % 2)
    y_peers = (lax.rem(my_cz + 4, N), lax.rem(my_cz + 12, N))
    signal(barrier, "kx", partner)
    signal(barrier, "cz", core_peer)
    signal(barrier, "cz", x_peer)
    for peer in y_peers:
        signal(barrier, "cz", peer)
    for upper in range(4, 8):
        near = jnp.logical_or(level == upper - 1, level == upper + 1)

        @pl.when(jnp.logical_or(level < (2 if upper == 7 else 4), near))
        def _():
            for c in range(2):
                signal(barrier, "kx", 2 * upper + c)
    loads = [
        pltpu.make_async_copy(src, dst, in_sem.at[i])
        for i, (src, dst) in enumerate((
            (fm_hbm, in_ref.at[0]), (ct_hbm, in_ref.at[1]),
            (h_hbm, h_ref), (st_hbm, st_ref), (pt_hbm, pt_ref)))
    ]
    for t in loads:
        t.start()
    r, c = iota((128, 128), 0), iota((128, 128), 1)
    perm_ref[...] = (c == (r % 8) * 16 + r // 8).astype(F32).astype(BF16)
    r, c = iota((512, 512), 0), iota((512, 512), 1)
    group_ref[...] = (c == (r % 4) * 128 + r // 4).astype(F32).astype(BF16)
    ends = jnp.logical_or(level == 4, level == 7)
    middle = jnp.logical_or(level == 5, level == 6)
    entered = jnp.where(ends, jnp.where(level == 7, 11, 15), jnp.where(middle, 17, jnp.where(level > 0, 6, 5)))
    pl.semaphore_wait(barrier, entered)

    @pl.when(level < 3)
    def _():
        signal(barrier, "kx", my_kx + 2)

    for lower in range(4):
        @pl.when(jnp.logical_and(level > lower, level < (8 if lower < 2 else 7)))
        def _():
            for c in range(2):
                signal(ready.at[level], "kx", 2 * lower + c)
    @pl.when(middle)
    def _():
        signal(chain.at[0], "kx", my_kx + 2)
        signal(chain.at[1], "kx", my_kx - 2)

    for peer in y_peers:
        signal(known.at[0], "cz", peer)

    def copy(stage, axis, src, dst, peer):
        return pltpu.make_async_remote_copy(
            src_ref=src.at[peer], dst_ref=dst.at[me[axis]],
            send_sem=ssem.at[stage], recv_sem=rsem.at[stage],
            device_id={axis: peer}, device_id_type=MESH,
        )

    def flipped(index, bits):
        for bit in (1, 2, 4, 8):
            if bits & bit:
                index = index + bit - 2 * bit * (index // bit % 2)
        return index

    def exchange(stage, axis, src, dst, by_index=False, first=()):
        for peer in first:
            @pl.when(me[axis] != peer)
            def _():
                copy(stage, axis, src, dst, peer).start()
        if by_index:
            for peer in range(N):
                @pl.when(me[axis] != peer)
                def _():
                    copy(stage, axis, src, dst, peer).start()
        else:
            flip = {0: me[axis]}
            for d in range(1, N):
                low = d & -d
                flip[d] = flipped(flip[d - low], low)
            for d in (10, 11, 14, 15, 6, 7, 8, 9, 2, 3, 12, 13, 4, 5, 1):
                if first:
                    @pl.when(flip[d] >= len(first))
                    def _():
                        copy(stage, axis, src, dst, flip[d]).start()
                else:
                    copy(stage, axis, src, dst, flip[d]).start()
        dst[me[axis]] = src[me[axis]]

    def wait_recv(stage, dst):
        pltpu.make_async_copy(dst.at[pl.ds(0, N - 1)], dst.at[pl.ds(0, N - 1)], rsem.at[stage]).wait()

    def wait_send(stage, src):
        pltpu.make_async_copy(src.at[pl.ds(0, N - 1)], src.at[pl.ds(0, N - 1)], ssem.at[stage]).wait()

    def to_level(arr, dest):
        for c in range(2):
            copy(arr, "kx", send1.at[arr], recv1.at[arr], 2 * dest + c).start()

    def prepare(arr):
        loads[arr].wait()
        parts = []
        for j in range(6):
            block = in_ref[arr, :, :, 128 * j:128 * (j + 1)].reshape(128, 128)
            parts.append(dot(perm_ref[...], block, NT).reshape(16, 8, 128))
        send1[arr] = jnp.concatenate(parts, axis=1).astype(BF16)

    def to_levels(arr, allowed):
        for d in (4, 3, 5, 2, 6, 1, 7):
            dest = lax.rem(level + d, 8)

            @pl.when(allowed(dest, d))
            def _():
                to_level(arr, dest)

    def to_partner(arr):
        copy(arr, "kx", send1.at[arr], recv1.at[arr], partner).start()
        recv1[arr, my_kx] = send1[arr, my_kx]

    def lower_ones(dest, d):
        low = jnp.logical_and(dest < jnp.where(level == 7, 2, 4), jnp.logical_or(level >= 4, dest < level))
        return jnp.logical_or(low, jnp.logical_and(level >= 4, dest >= 4)) if d in (1, 7) else low

    prepare(0)
    to_levels(0, lower_ones)
    to_partner(0)

    @pl.when(level == 7)
    def _():
        pl.semaphore_wait(chain.at[0], 1)
        for lower in (2, 3):
            for c in range(2):
                signal(ready.at[7], "kx", 2 * lower + c)
        for dest in (3, 2, 5):
            to_level(0, dest)

    prepare(1)

    @pl.when(level == 5)
    def _():
        pl.semaphore_wait(chain.at[1], 1)
        signal(chain.at[3], "kx", my_kx - 2)
        to_level(0, 7)

    @pl.when(level == 6)
    def _():
        pl.semaphore_wait(chain.at[0], 1)
        signal(chain.at[2], "kx", my_kx + 2)
        to_level(0, 4)

    @pl.when(level == 4)
    def _():
        pl.semaphore_wait(chain.at[1], 1)
        to_level(0, 6)
        pl.semaphore_wait(chain.at[3], 1)
        to_level(0, 7)

    @pl.when(level == 7)
    def _():
        pl.semaphore_wait(chain.at[2], 1)
        to_level(0, 4)

    def rest_of_b():
        to_levels(1, lambda dest, d: dest < jnp.where(level >= 4, 4, level))
        to_levels(1, lambda dest, d: jnp.logical_and(level >= 4, dest >= 4))

        @pl.when(level < 4)
        def _():
            for upper in range(1, 4):
                @pl.when(level < upper)
                def _():
                    to_level(1, upper)
            for upper in [
                jnp.where(level == 0, a, jnp.where(level == 1, b, jnp.where(level == 2, c, d)))
                for a, b, c, d in ((5, 6, 5, 6), (6, 5, 6, 5), (7, 7, 4, 4), (4, 4, 7, 7))
            ]:
                to_level(1, upper)
        to_partner(1)

    for upper in range(1, 4):
        @pl.when(level < upper)
        def _():
            pl.semaphore_wait(ready.at[upper], 2)
            to_level(0, upper)

    @pl.when(level < 4)
    def _():
        uppers = [
            jnp.where(level == 0, a, jnp.where(level == 1, b, jnp.where(level == 2, c, d)))
            for a, b, c, d in ((7, 7, 4, 4), (6, 4, 5, 5), (5, 6, 7, 6), (4, 5, 6, 7))
        ]
        for upper in uppers:
            pl.semaphore_wait(ready.at[upper], 2)
            to_level(0, upper)

    @pl.when(my_cz % 2 == 0)
    def _():
        rest_of_b()
    pl.semaphore_wait(known.at[0], 2)
    signal(known.at[1], "cz", x_peer)
    pl.semaphore_wait(known.at[1], 1)
    signal(known.at[2], "cz", core_peer)
    pl.semaphore_wait(known.at[2], 1)

    @pl.when(my_cz % 2 == 1)
    def _():
        rest_of_b()

    def transformed(i, got):
        rows = NX // PARTS
        return dot(h_ref[rows * i:rows * (i + 1)], got).astype(BF16).reshape(N // PARTS, XB, 128)

    for arr in range(2):
        if arr == 0:
            loads[2].wait()
        wait_recv(arr, recv1.at[arr])
        got = recv1[arr].reshape(NX, 128)
        for i in range(PARTS):
            send2[arr, 8 // PARTS * 2 * i:8 // PARTS * 2 * (i + 1)] = transformed(i, got)
        exchange(2 + arr, "cz", send2.at[arr], recv2.at[arr])

    loads[3].wait()
    loads[4].wait()
    for arr in range(2):
        wait_recv(2 + arr, recv2.at[arr])
        rows = jnp.concatenate(
            [jnp.concatenate([recv2[arr, 4 * g + i] for i in range(4)], axis=1) for g in range(4)],
            axis=0,
        )
        rows = dot(rows, group_ref[...]).astype(BF16)
        rows = jnp.concatenate(
            [
                jnp.concatenate(
                    [rows[XB * g:XB * (g + 1), 128 * f:128 * (f + 1)] for g in range(4)], axis=1)
                for f in range(4)
            ],
            axis=0,
        )
        table = (st_ref, pt_ref)[arr]
        lift_ref[arr] = dot(rows, table[...]).reshape(4, XB, MZ)

    u, v, w, b = (lift_ref[0, f] for f in range(4))
    au, av, aw, ab = (lift_ref[1, f] for f in range(4))
    grad = jnp.concatenate(
        [
            (au * w).astype(BF16),
            (av * w).astype(BF16),
            (au * u + av * v + 2.0 * aw * w + ab * b).astype(BF16),
            (ab * w).astype(BF16),
        ],
        axis=0,
    )
    back = dot(grad, st_ref[...], NT).astype(BF16)
    back = jnp.concatenate(
        [
            jnp.concatenate(
                [back[XB * f:XB * (f + 1), 128 * g:128 * (g + 1)] for f in range(4)], axis=1)
            for g in range(4)
        ],
        axis=0,
    )
    back = dot(back, group_ref[...], NT).astype(BF16)
    for g in range(4):
        for i in range(4):
            send3[4 * g + i] = back[XB * g:XB * (g + 1), 128 * i:128 * (i + 1)]
    exchange(4, "cz", send3, recv3, first=(0, 1))
    wait_recv(4, recv3)
    got = recv3[...].reshape(NX, 128)
    for i in range(PARTS):
        send4[8 // PARTS * 2 * i:8 // PARTS * 2 * (i + 1)] = transformed(i, got)
    exchange(5, "kx", send4, recv4, by_index=True)
    wait_recv(5, recv4)
    out_ref[...] = recv4[...]
    for arr in range(2):
        wait_send(arr, send1.at[arr])
        wait_send(2 + arr, send2.at[arr])
    wait_send(4, send3)
    wait_send(5, send4)


def unpack(in_ref, out_ref):
    r, c = iota((128, 128), 0), iota((128, 128), 1)
    perm = (c == (r % 8) * 16 + r // 8).astype(F32).astype(BF16)
    got = in_ref[...].astype(F32)
    for j in range(6):
        block = got[:, 8 * j:8 * (j + 1), :].reshape(128, 128).astype(BF16)
        out_ref[:, :, 128 * j:128 * (j + 1)] = dot(block, perm, TN).astype(BF16).reshape(32, 4, 128)


def on_device(field_modes, cotangent):
    cosines = cosine_table()
    synthesis = jnp.asarray((cosines * math.sqrt(2.0 / NZ)).astype(BF16).T)
    projection = jnp.asarray((cosines * math.sqrt(2.0 / MZ)).astype(BF16).T)
    hartley = jnp.asarray(hartley_table())
    vmem = pl.BlockSpec(memory_space=pltpu.VMEM)
    hbm = pl.BlockSpec(memory_space=pl.ANY)
    one = pltpu.VMEM((N, XB, 128), BF16)
    two = pltpu.VMEM((2, N, XB, 128), BF16)
    blocks = pl.pallas_call(
        kernel,
        out_shape=pltpu.VMEM((N, XB, 128), BF16),
        in_specs=[hbm] * 5,
        out_specs=vmem,
        scratch_shapes=[
            pltpu.VMEM((2,) + field_modes.shape, BF16),
            pltpu.VMEM((NX, NX), BF16),
            pltpu.VMEM((NZ, MZ), BF16),
            pltpu.VMEM((NZ, MZ), BF16),
            two, two, two, two, one, one, one, one,
            pltpu.VMEM((2, 4, XB, MZ), F32),
            pltpu.VMEM((128, 128), BF16),
            pltpu.VMEM((512, 512), BF16),
            pltpu.SemaphoreType.DMA((5,)),
            pltpu.SemaphoreType.DMA((6,)),
            pltpu.SemaphoreType.DMA((6,)),
            pltpu.SemaphoreType.REGULAR((8,)),
            pltpu.SemaphoreType.REGULAR((3,)),
            pltpu.SemaphoreType.REGULAR((4,)),
        ],
        compiler_params=pltpu.CompilerParams(collective_id=0, has_side_effects=True),
    )(field_modes, cotangent, hartley, synthesis, projection)
    return pl.pallas_call(
        unpack,
        out_shape=jax.ShapeDtypeStruct(field_modes.shape, BF16),
        in_specs=[vmem],
        out_specs=vmem,
    )(pltpu.with_memory_space_constraint(blocks, pltpu.VMEM))


def solution(mesh):
    return jax.shard_map(
        on_device,
        mesh=mesh,
        in_specs=(P("cz", None, "kx"), P("cz", None, "kx")),
        out_specs=P("cz", None, "kx"),
        check_vma=False,
    )
```

```python
import math

import jax
import jax.numpy as jnp
import numpy as np
from jax import lax
from jax.experimental import pallas as pl
from jax.experimental.pallas import tpu as pltpu
from jax.sharding import PartitionSpec as P

NZ = 512
MZ = 768
NX = 768
Y = 16
N = 16
XB = NX // N
PARTS = 4
MESH = pl.DeviceIdType.MESH
F32 = jnp.float32
BF16 = jnp.bfloat16
NT = (((1,), (1,)), ((), ()))
TN = (((0,), (0,)), ((), ()))


def cosine_table():
    row_index = np.arange(MZ, dtype=np.int32)
    col_index = np.arange(NZ, dtype=np.int32)
    position = col_index[None, :] * (2 * row_index[:, None] + 1) % (4 * MZ)
    return np.cos(np.pi * position / (2 * MZ)).astype(np.float32)


def hartley_table():
    points = np.arange(NX, dtype=np.int32)
    position = points[:, None] * points[None, :] % NX
    phases = 2.0 * np.pi * position / NX
    return ((np.cos(phases) + np.sin(phases)) / math.sqrt(NX)).astype(BF16)


def iota(shape, dim):
    return lax.broadcasted_iota(jnp.int32, shape, dim)


def dot(a, b, dims=(((1,), (0,)), ((), ()))):
    return lax.dot_general(a, b, dims, preferred_element_type=F32)


def kernel(
    fm_hbm, ct_hbm, h_hbm, st_hbm, pt_hbm, out_ref,
    in_ref, h_ref, st_ref, pt_ref, send1, recv1, send2, recv2, send3, recv3, send4, recv4,
    lift_ref, perm_ref, group_ref, in_sem, ssem, rsem, ready, known, chain,
):
    my_kx = lax.axis_index("kx")
    my_cz = lax.axis_index("cz")
    me = {"kx": my_kx, "cz": my_cz}
    level, side = my_kx // 2, my_kx % 2

    def signal(sem, axis, peer):
        pl.semaphore_signal(sem, inc=1, device_id={axis: peer}, device_id_type=MESH)

    barrier = pltpu.get_barrier_semaphore()
    partner = my_kx + 1 - 2 * side
    core_peer = my_cz + 1 - 2 * (my_cz % 2)
    x_peer = my_cz + 2 - 4 * (my_cz // 2 % 2)
    y_peers = (lax.rem(my_cz + 4, N), lax.rem(my_cz + 12, N))
    signal(barrier, "kx", partner)
    signal(barrier, "cz", core_peer)
    signal(barrier, "cz", x_peer)
    for peer in y_peers:
        signal(barrier, "cz", peer)
    for upper in range(4, 8):
        near = jnp.logical_or(level == upper - 1, level == upper + 1)

        @pl.when(jnp.logical_or(level < (2 if upper == 7 else 4), near))
        def _():
            for c in range(2):
                signal(barrier, "kx", 2 * upper + c)
    loads = [
        pltpu.make_async_copy(src, dst, in_sem.at[i])
        for i, (src, dst) in enumerate((
            (fm_hbm, in_ref.at[0]), (ct_hbm, in_ref.at[1]),
            (h_hbm, h_ref), (st_hbm, st_ref), (pt_hbm, pt_ref)))
    ]
    for t in loads:
        t.start()
    r, c = iota((128, 128), 0), iota((128, 128), 1)
    perm_ref[...] = (c == (r % 8) * 16 + r // 8).astype(F32).astype(BF16)
    r, c = iota((512, 512), 0), iota((512, 512), 1)
    group_ref[...] = (c == (r % 4) * 128 + r // 4).astype(F32).astype(BF16)
    ends = jnp.logical_or(level == 4, level == 7)
    middle = jnp.logical_or(level == 5, level == 6)
    entered = jnp.where(ends, jnp.where(level == 7, 11, 15), jnp.where(middle, 17, jnp.where(level > 0, 6, 5)))
    pl.semaphore_wait(barrier, entered)

    @pl.when(level < 3)
    def _():
        signal(barrier, "kx", my_kx + 2)

    for lower in range(4):
        @pl.when(jnp.logical_and(level > lower, level < (8 if lower < 2 else 7)))
        def _():
            for c in range(2):
                signal(ready.at[level], "kx", 2 * lower + c)
    @pl.when(middle)
    def _():
        signal(chain.at[0], "kx", my_kx + 2)
        signal(chain.at[1], "kx", my_kx - 2)

    for peer in y_peers:
        signal(known.at[0], "cz", peer)

    def copy(stage, axis, src, dst, peer):
        return pltpu.make_async_remote_copy(
            src_ref=src.at[peer], dst_ref=dst.at[me[axis]],
            send_sem=ssem.at[stage], recv_sem=rsem.at[stage],
            device_id={axis: peer}, device_id_type=MESH,
        )

    def flipped(index, bits):
        for bit in (1, 2, 4, 8):
            if bits & bit:
                index = index + bit - 2 * bit * (index // bit % 2)
        return index

    def exchange(stage, axis, src, dst, by_index=False, first=()):
        for peer in first:
            @pl.when(me[axis] != peer)
            def _():
                copy(stage, axis, src, dst, peer).start()
        if by_index:
            for peer in range(N):
                peer = lax.rem(peer + jnp.where(level < 4, 8, 0), N)

                @pl.when(me[axis] != peer)
                def _():
                    copy(stage, axis, src, dst, peer).start()
        else:
            flip = {0: me[axis]}
            for d in range(1, N):
                low = d & -d
                flip[d] = flipped(flip[d - low], low)
            for d in (10, 11, 14, 15, 6, 7, 8, 9, 2, 3, 12, 13, 4, 5, 1):
                if first:
                    @pl.when(flip[d] >= len(first))
                    def _():
                        copy(stage, axis, src, dst, flip[d]).start()
                else:
                    copy(stage, axis, src, dst, flip[d]).start()
        dst[me[axis]] = src[me[axis]]

    def wait_recv(stage, dst):
        pltpu.make_async_copy(dst.at[pl.ds(0, N - 1)], dst.at[pl.ds(0, N - 1)], rsem.at[stage]).wait()

    def wait_send(stage, src):
        pltpu.make_async_copy(src.at[pl.ds(0, N - 1)], src.at[pl.ds(0, N - 1)], ssem.at[stage]).wait()

    def to_level(arr, dest):
        for c in range(2):
            copy(arr, "kx", send1.at[arr], recv1.at[arr], 2 * dest + c).start()

    def prepare(arr):
        loads[arr].wait()
        parts = []
        for j in range(6):
            block = in_ref[arr, :, :, 128 * j:128 * (j + 1)].reshape(128, 128)
            parts.append(dot(perm_ref[...], block, NT).reshape(16, 8, 128))
        send1[arr] = jnp.concatenate(parts, axis=1).astype(BF16)

    def to_levels(arr, allowed):
        for d in (4, 3, 5, 2, 6, 1, 7):
            dest = lax.rem(level + d, 8)

            @pl.when(allowed(dest, d))
            def _():
                to_level(arr, dest)

    def to_partner(arr):
        copy(arr, "kx", send1.at[arr], recv1.at[arr], partner).start()
        recv1[arr, my_kx] = send1[arr, my_kx]

    def lower_ones(dest, d):
        low = jnp.logical_and(dest < jnp.where(level == 7, 2, 4), jnp.logical_or(level >= 4, dest < level))
        return jnp.logical_or(low, jnp.logical_and(level >= 4, dest >= 4)) if d in (1, 7) else low

    prepare(0)
    to_levels(0, lower_ones)
    to_partner(0)

    @pl.when(level == 7)
    def _():
        pl.semaphore_wait(chain.at[0], 1)
        for lower in (2, 3):
            for c in range(2):
                signal(ready.at[7], "kx", 2 * lower + c)
        for dest in (3, 2, 5):
            to_level(0, dest)

    prepare(1)

    @pl.when(level == 5)
    def _():
        pl.semaphore_wait(chain.at[1], 1)
        signal(chain.at[3], "kx", my_kx - 2)
        to_level(0, 7)

    @pl.when(level == 6)
    def _():
        pl.semaphore_wait(chain.at[0], 1)
        signal(chain.at[2], "kx", my_kx + 2)
        to_level(0, 4)

    @pl.when(level == 4)
    def _():
        pl.semaphore_wait(chain.at[1], 1)
        to_level(0, 6)
        pl.semaphore_wait(chain.at[3], 1)
        to_level(0, 7)

    @pl.when(level == 7)
    def _():
        pl.semaphore_wait(chain.at[2], 1)
        to_level(0, 4)

    def rest_of_b():
        to_levels(1, lambda dest, d: dest < jnp.where(level >= 4, 4, level))
        to_levels(1, lambda dest, d: jnp.logical_and(level >= 4, dest >= 4))

        @pl.when(level < 4)
        def _():
            for upper in range(1, 4):
                @pl.when(level < upper)
                def _():
                    to_level(1, upper)
            for upper in [
                jnp.where(level == 0, a, jnp.where(level == 1, b, jnp.where(level == 2, c, d)))
                for a, b, c, d in ((4, 4, 7, 7), (5, 5, 6, 6), (6, 6, 5, 5), (7, 7, 4, 4))
            ]:
                to_level(1, upper)
        to_partner(1)

    for upper in range(1, 4):
        @pl.when(level < upper)
        def _():
            pl.semaphore_wait(ready.at[upper], 2)
            to_level(0, upper)

    @pl.when(level < 4)
    def _():
        uppers = [
            jnp.where(level == 0, a, jnp.where(level == 1, b, jnp.where(level == 2, c, d)))
            for a, b, c, d in ((7, 7, 4, 4), (6, 4, 5, 5), (5, 6, 7, 6), (4, 5, 6, 7))
        ]
        for upper in uppers:
            pl.semaphore_wait(ready.at[upper], 2)
            to_level(0, upper)

    @pl.when(my_cz % 2 == 0)
    def _():
        rest_of_b()
    pl.semaphore_wait(known.at[0], 2)
    signal(known.at[1], "cz", x_peer)
    pl.semaphore_wait(known.at[1], 1)
    signal(known.at[2], "cz", core_peer)
    pl.semaphore_wait(known.at[2], 1)

    @pl.when(my_cz % 2 == 1)
    def _():
        rest_of_b()

    def transformed(i, got):
        rows = NX // PARTS
        return dot(h_ref[rows * i:rows * (i + 1)], got).astype(BF16).reshape(N // PARTS, XB, 128)

    for arr in range(2):
        if arr == 0:
            loads[2].wait()
        wait_recv(arr, recv1.at[arr])
        got = recv1[arr].reshape(NX, 128)
        for i in range(PARTS):
            send2[arr, 8 // PARTS * 2 * i:8 // PARTS * 2 * (i + 1)] = transformed(i, got)
        exchange(2 + arr, "cz", send2.at[arr], recv2.at[arr])

    loads[3].wait()
    loads[4].wait()
    for arr in range(2):
        wait_recv(2 + arr, recv2.at[arr])
        rows = jnp.concatenate(
            [jnp.concatenate([recv2[arr, 4 * g + i] for i in range(4)], axis=1) for g in range(4)],
            axis=0,
        )
        rows = dot(rows, group_ref[...]).astype(BF16)
        rows = jnp.concatenate(
            [
                jnp.concatenate(
                    [rows[XB * g:XB * (g + 1), 128 * f:128 * (f + 1)] for g in range(4)], axis=1)
                for f in range(4)
            ],
            axis=0,
        )
        table = (st_ref, pt_ref)[arr]
        lift_ref[arr] = dot(rows, table[...]).reshape(4, XB, MZ)

    u, v, w, b = (lift_ref[0, f] for f in range(4))
    au, av, aw, ab = (lift_ref[1, f] for f in range(4))
    grad = jnp.concatenate(
        [
            (au * w).astype(BF16),
            (av * w).astype(BF16),
            (au * u + av * v + 2.0 * aw * w + ab * b).astype(BF16),
            (ab * w).astype(BF16),
        ],
        axis=0,
    )
    back = dot(grad, st_ref[...], NT).astype(BF16)
    back = jnp.concatenate(
        [
            jnp.concatenate(
                [back[XB * f:XB * (f + 1), 128 * g:128 * (g + 1)] for f in range(4)], axis=1)
            for g in range(4)
        ],
        axis=0,
    )
    back = dot(back, group_ref[...], NT).astype(BF16)
    for g in range(4):
        for i in range(4):
            send3[4 * g + i] = back[XB * g:XB * (g + 1), 128 * i:128 * (i + 1)]
    exchange(4, "cz", send3, recv3, first=(0, 1))
    wait_recv(4, recv3)
    got = recv3[...].reshape(NX, 128)
    for i in range(PARTS):
        send4[8 // PARTS * 2 * i:8 // PARTS * 2 * (i + 1)] = transformed(i, got)
    exchange(5, "kx", send4, recv4, by_index=True)
    wait_recv(5, recv4)
    out_ref[...] = recv4[...]
    for arr in range(2):
        wait_send(arr, send1.at[arr])
        wait_send(2 + arr, send2.at[arr])
    wait_send(4, send3)
    wait_send(5, send4)


def unpack(in_ref, out_ref):
    r, c = iota((128, 128), 0), iota((128, 128), 1)
    perm = (c == (r % 8) * 16 + r // 8).astype(F32).astype(BF16)
    got = in_ref[...].astype(F32)
    for j in range(6):
        block = got[:, 8 * j:8 * (j + 1), :].reshape(128, 128).astype(BF16)
        out_ref[:, :, 128 * j:128 * (j + 1)] = dot(block, perm, TN).astype(BF16).reshape(32, 4, 128)


def on_device(field_modes, cotangent):
    cosines = cosine_table()
    synthesis = jnp.asarray((cosines * math.sqrt(2.0 / NZ)).astype(BF16).T)
    projection = jnp.asarray((cosines * math.sqrt(2.0 / MZ)).astype(BF16).T)
    hartley = jnp.asarray(hartley_table())
    vmem = pl.BlockSpec(memory_space=pltpu.VMEM)
    hbm = pl.BlockSpec(memory_space=pl.ANY)
    one = pltpu.VMEM((N, XB, 128), BF16)
    two = pltpu.VMEM((2, N, XB, 128), BF16)
    blocks = pl.pallas_call(
        kernel,
        out_shape=pltpu.VMEM((N, XB, 128), BF16),
        in_specs=[hbm] * 5,
        out_specs=vmem,
        scratch_shapes=[
            pltpu.VMEM((2,) + field_modes.shape, BF16),
            pltpu.VMEM((NX, NX), BF16),
            pltpu.VMEM((NZ, MZ), BF16),
            pltpu.VMEM((NZ, MZ), BF16),
            two, two, two, two, one, one, one, one,
            pltpu.VMEM((2, 4, XB, MZ), F32),
            pltpu.VMEM((128, 128), BF16),
            pltpu.VMEM((512, 512), BF16),
            pltpu.SemaphoreType.DMA((5,)),
            pltpu.SemaphoreType.DMA((6,)),
            pltpu.SemaphoreType.DMA((6,)),
            pltpu.SemaphoreType.REGULAR((8,)),
            pltpu.SemaphoreType.REGULAR((3,)),
            pltpu.SemaphoreType.REGULAR((4,)),
        ],
        compiler_params=pltpu.CompilerParams(collective_id=0, has_side_effects=True),
    )(field_modes, cotangent, hartley, synthesis, projection)
    return pl.pallas_call(
        unpack,
        out_shape=jax.ShapeDtypeStruct(field_modes.shape, BF16),
        in_specs=[vmem],
        out_specs=vmem,
    )(pltpu.with_memory_space_constraint(blocks, pltpu.VMEM))


def solution(mesh):
    return jax.shard_map(
        on_device,
        mesh=mesh,
        in_specs=(P("cz", None, "kx"), P("cz", None, "kx")),
        out_specs=P("cz", None, "kx"),
        check_vma=False,
    )
```

```python
import math

import jax
import jax.numpy as jnp
import numpy as np
from jax import lax
from jax.experimental import pallas as pl
from jax.experimental.pallas import tpu as pltpu
from jax.sharding import PartitionSpec as P

NZ = 512
MZ = 768
NX = 768
Y = 16
N = 16
XB = NX // N
PARTS = 4
MESH = pl.DeviceIdType.MESH
F32 = jnp.float32
BF16 = jnp.bfloat16
NT = (((1,), (1,)), ((), ()))
TN = (((0,), (0,)), ((), ()))


def cosine_table():
    row_index = np.arange(MZ, dtype=np.int32)
    col_index = np.arange(NZ, dtype=np.int32)
    position = col_index[None, :] * (2 * row_index[:, None] + 1) % (4 * MZ)
    return np.cos(np.pi * position / (2 * MZ)).astype(np.float32)


def hartley_table():
    points = np.arange(NX, dtype=np.int32)
    position = points[:, None] * points[None, :] % NX
    phases = 2.0 * np.pi * position / NX
    return ((np.cos(phases) + np.sin(phases)) / math.sqrt(NX)).astype(BF16)


def iota(shape, dim):
    return lax.broadcasted_iota(jnp.int32, shape, dim)


def dot(a, b, dims=(((1,), (0,)), ((), ()))):
    return lax.dot_general(a, b, dims, preferred_element_type=F32)


def kernel(
    fm_hbm, ct_hbm, h_hbm, st_hbm, pt_hbm, out_ref,
    in_ref, h_ref, st_ref, pt_ref, send1, recv1, send2, recv2, send3, recv3, send4, recv4,
    lift_ref, perm_ref, group_ref, in_sem, ssem, rsem, ready, known, chain,
):
    my_kx = lax.axis_index("kx")
    my_cz = lax.axis_index("cz")
    me = {"kx": my_kx, "cz": my_cz}
    level, side = my_kx // 2, my_kx % 2

    def signal(sem, axis, peer):
        pl.semaphore_signal(sem, inc=1, device_id={axis: peer}, device_id_type=MESH)

    barrier = pltpu.get_barrier_semaphore()
    partner = my_kx + 1 - 2 * side
    core_peer = my_cz + 1 - 2 * (my_cz % 2)
    x_peer = my_cz + 2 - 4 * (my_cz // 2 % 2)
    y_peers = (lax.rem(my_cz + 4, N), lax.rem(my_cz + 12, N))
    signal(barrier, "kx", partner)

    @pl.when(level < 4)
    def _():
        signal(barrier, "cz", core_peer)
        signal(barrier, "cz", x_peer)
        for peer in y_peers:
            signal(barrier, "cz", peer)

    for upper in range(4, 8):
        near = jnp.logical_or(level == upper - 1, level == upper + 1)

        @pl.when(jnp.logical_or(level < (2 if upper == 7 else 4), near))
        def _():
            for c in range(2):
                signal(barrier, "kx", 2 * upper + c)
    loads = [
        pltpu.make_async_copy(src, dst, in_sem.at[i])
        for i, (src, dst) in enumerate((
            (fm_hbm, in_ref.at[0]), (ct_hbm, in_ref.at[1]),
            (h_hbm, h_ref), (st_hbm, st_ref), (pt_hbm, pt_ref)))
    ]
    for t in loads:
        t.start()
    r, c = iota((128, 128), 0), iota((128, 128), 1)
    perm_ref[...] = (c == (r % 8) * 16 + r // 8).astype(F32).astype(BF16)
    r, c = iota((512, 512), 0), iota((512, 512), 1)
    group_ref[...] = (c == (r % 4) * 128 + r // 4).astype(F32).astype(BF16)
    ends = jnp.logical_or(level == 4, level == 7)
    middle = jnp.logical_or(level == 5, level == 6)
    entered = jnp.where(ends, jnp.where(level == 7, 7, 11), jnp.where(middle, 13, jnp.where(level > 0, 6, 5)))
    pl.semaphore_wait(barrier, entered)

    @pl.when(level < 3)
    def _():
        signal(barrier, "kx", my_kx + 2)

    for lower in range(4):
        @pl.when(jnp.logical_and(level > lower, level < (8 if lower < 2 else 7)))
        def _():
            for c in range(2):
                signal(ready.at[level], "kx", 2 * lower + c)
    @pl.when(middle)
    def _():
        signal(chain.at[0], "kx", my_kx + 2)
        signal(chain.at[1], "kx", my_kx - 2)


    def copy(stage, axis, src, dst, peer):
        return pltpu.make_async_remote_copy(
            src_ref=src.at[peer], dst_ref=dst.at[me[axis]],
            send_sem=ssem.at[stage], recv_sem=rsem.at[stage],
            device_id={axis: peer}, device_id_type=MESH,
        )

    def flipped(index, bits):
        for bit in (1, 2, 4, 8):
            if bits & bit:
                index = index + bit - 2 * bit * (index // bit % 2)
        return index

    def exchange(stage, axis, src, dst, by_index=False, first=()):
        for peer in first:
            @pl.when(me[axis] != peer)
            def _():
                copy(stage, axis, src, dst, peer).start()
        if by_index:
            for peer in range(N):
                peer = lax.rem(peer + jnp.where(level < 4, 8, 0), N)

                @pl.when(me[axis] != peer)
                def _():
                    copy(stage, axis, src, dst, peer).start()
        else:
            flip = {0: me[axis]}
            for d in range(1, N):
                low = d & -d
                flip[d] = flipped(flip[d - low], low)
            for d in (10, 11, 14, 15, 6, 7, 8, 9, 2, 3, 12, 13, 4, 5, 1):
                if first:
                    @pl.when(flip[d] >= len(first))
                    def _():
                        copy(stage, axis, src, dst, flip[d]).start()
                else:
                    copy(stage, axis, src, dst, flip[d]).start()
        dst[me[axis]] = src[me[axis]]

    def wait_recv(stage, dst):
        pltpu.make_async_copy(dst.at[pl.ds(0, N - 1)], dst.at[pl.ds(0, N - 1)], rsem.at[stage]).wait()

    def wait_send(stage, src):
        pltpu.make_async_copy(src.at[pl.ds(0, N - 1)], src.at[pl.ds(0, N - 1)], ssem.at[stage]).wait()

    def to_level(arr, dest):
        for c in range(2):
            copy(arr, "kx", send1.at[arr], recv1.at[arr], 2 * dest + c).start()

    def prepare(arr):
        loads[arr].wait()
        parts = []
        for j in range(6):
            block = in_ref[arr, :, :, 128 * j:128 * (j + 1)].reshape(128, 128)
            parts.append(dot(perm_ref[...], block, NT).reshape(16, 8, 128))
        send1[arr] = jnp.concatenate(parts, axis=1).astype(BF16)

    def to_levels(arr, allowed):
        for d in (4, 3, 5, 2, 6, 1, 7):
            dest = lax.rem(level + d, 8)

            @pl.when(allowed(dest, d))
            def _():
                to_level(arr, dest)

    def to_partner(arr):
        copy(arr, "kx", send1.at[arr], recv1.at[arr], partner).start()
        recv1[arr, my_kx] = send1[arr, my_kx]

    def lower_ones(dest, d):
        low = jnp.logical_and(dest < jnp.where(level == 7, 2, 4), jnp.logical_or(level >= 4, dest < level))
        return jnp.logical_or(low, jnp.logical_and(level >= 4, dest >= 4)) if d in (1, 7) else low

    prepare(0)
    to_levels(0, lower_ones)
    to_partner(0)

    @pl.when(level == 7)
    def _():
        pl.semaphore_wait(chain.at[0], 1)
        for lower in (2, 3):
            for c in range(2):
                signal(ready.at[7], "kx", 2 * lower + c)
        for dest in (3, 2, 5):
            to_level(0, dest)

    prepare(1)

    @pl.when(level == 5)
    def _():
        pl.semaphore_wait(chain.at[1], 1)
        signal(chain.at[3], "kx", my_kx - 2)
        to_level(0, 7)

    @pl.when(level == 6)
    def _():
        pl.semaphore_wait(chain.at[0], 1)
        signal(chain.at[2], "kx", my_kx + 2)
        to_level(0, 4)

    @pl.when(level == 4)
    def _():
        pl.semaphore_wait(chain.at[1], 1)
        to_level(0, 6)
        pl.semaphore_wait(chain.at[3], 1)
        to_level(0, 7)

    @pl.when(level == 7)
    def _():
        pl.semaphore_wait(chain.at[2], 1)
        to_level(0, 4)

    def rest_of_b():
        to_levels(1, lambda dest, d: dest < jnp.where(level >= 4, 4, level))
        to_levels(1, lambda dest, d: jnp.logical_and(level >= 4, dest >= 4))

        @pl.when(level < 4)
        def _():
            for upper in range(1, 4):
                @pl.when(level < upper)
                def _():
                    to_level(1, upper)
            for upper in [
                jnp.where(level == 0, a, jnp.where(level == 1, b, jnp.where(level == 2, c, d)))
                for a, b, c, d in ((4, 4, 7, 7), (5, 5, 6, 6), (6, 6, 5, 5), (7, 7, 4, 4))
            ]:
                to_level(1, upper)
        to_partner(1)

    for upper in range(1, 4):
        @pl.when(level < upper)
        def _():
            pl.semaphore_wait(ready.at[upper], 2)
            to_level(0, upper)

    @pl.when(level < 4)
    def _():
        uppers = [
            jnp.where(level == 0, a, jnp.where(level == 1, b, jnp.where(level == 2, c, d)))
            for a, b, c, d in ((7, 7, 4, 4), (6, 4, 5, 5), (5, 6, 7, 6), (4, 5, 6, 7))
        ]
        for upper in uppers:
            pl.semaphore_wait(ready.at[upper], 2)
            to_level(0, upper)

    @pl.when(my_cz % 2 == 0)
    def _():
        rest_of_b()

    @pl.when(level < 4)
    def _():
        for turn in range(2):
            for peer in y_peers:
                signal(known.at[turn], "cz", peer)
            pl.semaphore_wait(known.at[turn], 2)
            if turn == 0:
                @pl.when(my_cz % 2 == 1)
                def _():
                    rest_of_b()
        signal(known.at[2], "cz", x_peer)
        pl.semaphore_wait(known.at[2], 1)
        signal(known.at[3], "cz", core_peer)
        pl.semaphore_wait(known.at[3], 1)
        for lower, uppers in ((0, (7, 6)), (3, (4, 5))):
            @pl.when(level == lower)
            def _():
                for upper in uppers:
                    signal(known.at[4], "kx", 2 * upper + side)

    def transformed(i, got):
        rows = NX // PARTS
        return dot(h_ref[rows * i:rows * (i + 1)], got).astype(BF16).reshape(N // PARTS, XB, 128)

    for arr in range(2):
        if arr == 0:
            loads[2].wait()
        wait_recv(arr, recv1.at[arr])
        if arr == 0:
            @pl.when(jnp.logical_and(level >= 4, my_cz % 2 == 1))
            def _():
                rest_of_b()
        got = recv1[arr].reshape(NX, 128)
        for i in range(PARTS):
            send2[arr, 8 // PARTS * 2 * i:8 // PARTS * 2 * (i + 1)] = transformed(i, got)
        if arr == 0:
            @pl.when(level >= 4)
            def _():
                pl.semaphore_wait(known.at[4], 1)
        exchange(2 + arr, "cz", send2.at[arr], recv2.at[arr])

    loads[3].wait()
    loads[4].wait()
    for arr in range(2):
        wait_recv(2 + arr, recv2.at[arr])
        rows = jnp.concatenate(
            [jnp.concatenate([recv2[arr, 4 * g + i] for i in range(4)], axis=1) for g in range(4)],
            axis=0,
        )
        rows = dot(rows, group_ref[...]).astype(BF16)
        rows = jnp.concatenate(
            [
                jnp.concatenate(
                    [rows[XB * g:XB * (g + 1), 128 * f:128 * (f + 1)] for g in range(4)], axis=1)
                for f in range(4)
            ],
            axis=0,
        )
        table = (st_ref, pt_ref)[arr]
        lift_ref[arr] = dot(rows, table[...]).reshape(4, XB, MZ)

    u, v, w, b = (lift_ref[0, f] for f in range(4))
    au, av, aw, ab = (lift_ref[1, f] for f in range(4))
    grad = jnp.concatenate(
        [
            (au * w).astype(BF16),
            (av * w).astype(BF16),
            (au * u + av * v + 2.0 * aw * w + ab * b).astype(BF16),
            (ab * w).astype(BF16),
        ],
        axis=0,
    )
    back = dot(grad, st_ref[...], NT).astype(BF16)
    back = jnp.concatenate(
        [
            jnp.concatenate(
                [back[XB * f:XB * (f + 1), 128 * g:128 * (g + 1)] for f in range(4)], axis=1)
            for g in range(4)
        ],
        axis=0,
    )
    back = dot(back, group_ref[...], NT).astype(BF16)
    for g in range(4):
        for i in range(4):
            send3[4 * g + i] = back[XB * g:XB * (g + 1), 128 * i:128 * (i + 1)]
    exchange(4, "cz", send3, recv3, first=(0, 1))
    wait_recv(4, recv3)
    got = recv3[...].reshape(NX, 128)
    for i in range(PARTS):
        send4[8 // PARTS * 2 * i:8 // PARTS * 2 * (i + 1)] = transformed(i, got)
    exchange(5, "kx", send4, recv4, by_index=True)
    wait_recv(5, recv4)
    out_ref[...] = recv4[...]
    for arr in range(2):
        wait_send(arr, send1.at[arr])
        wait_send(2 + arr, send2.at[arr])
    wait_send(4, send3)
    wait_send(5, send4)


def unpack(in_ref, out_ref):
    r, c = iota((128, 128), 0), iota((128, 128), 1)
    perm = (c == (r % 8) * 16 + r // 8).astype(F32).astype(BF16)
    got = in_ref[...].astype(F32)
    for j in range(6):
        block = got[:, 8 * j:8 * (j + 1), :].reshape(128, 128).astype(BF16)
        out_ref[:, :, 128 * j:128 * (j + 1)] = dot(block, perm, TN).astype(BF16).reshape(32, 4, 128)


def on_device(field_modes, cotangent):
    cosines = cosine_table()
    synthesis = jnp.asarray((cosines * math.sqrt(2.0 / NZ)).astype(BF16).T)
    projection = jnp.asarray((cosines * math.sqrt(2.0 / MZ)).astype(BF16).T)
    hartley = jnp.asarray(hartley_table())
    vmem = pl.BlockSpec(memory_space=pltpu.VMEM)
    hbm = pl.BlockSpec(memory_space=pl.ANY)
    one = pltpu.VMEM((N, XB, 128), BF16)
    two = pltpu.VMEM((2, N, XB, 128), BF16)
    blocks = pl.pallas_call(
        kernel,
        out_shape=pltpu.VMEM((N, XB, 128), BF16),
        in_specs=[hbm] * 5,
        out_specs=vmem,
        scratch_shapes=[
            pltpu.VMEM((2,) + field_modes.shape, BF16),
            pltpu.VMEM((NX, NX), BF16),
            pltpu.VMEM((NZ, MZ), BF16),
            pltpu.VMEM((NZ, MZ), BF16),
            two, two, two, two, one, one, one, one,
            pltpu.VMEM((2, 4, XB, MZ), F32),
            pltpu.VMEM((128, 128), BF16),
            pltpu.VMEM((512, 512), BF16),
            pltpu.SemaphoreType.DMA((5,)),
            pltpu.SemaphoreType.DMA((6,)),
            pltpu.SemaphoreType.DMA((6,)),
            pltpu.SemaphoreType.REGULAR((8,)),
            pltpu.SemaphoreType.REGULAR((5,)),
            pltpu.SemaphoreType.REGULAR((4,)),
        ],
        compiler_params=pltpu.CompilerParams(collective_id=0, has_side_effects=True),
    )(field_modes, cotangent, hartley, synthesis, projection)
    return pl.pallas_call(
        unpack,
        out_shape=jax.ShapeDtypeStruct(field_modes.shape, BF16),
        in_specs=[vmem],
        out_specs=vmem,
    )(pltpu.with_memory_space_constraint(blocks, pltpu.VMEM))


def solution(mesh):
    return jax.shard_map(
        on_device,
        mesh=mesh,
        in_specs=(P("cz", None, "kx"), P("cz", None, "kx")),
        out_specs=P("cz", None, "kx"),
        check_vma=False,
    )
```
